512 devices in a mesh: unit: 2 (over y_1), row: 16 (over y_0, x, core), col: 16 (over z, y_2).
Axes of the slice: x: 4, y: 8 (y_0: 2, y_1: 2, y_2: 2; y = y_0 * 4 + y_1 * 2 + y_2), z: 8, core: 2. Of those that a mesh axis runs over, the one named last changes fastest.
Arguments:
- tracer: float32 [4, 128, 256, 256], P('unit', None, 'row', 'col'), parts along dimension 0, may hold values from -6 to 6
- symbol_x: float32 [128], replicated, may hold values from 0.3 to 3
- symbol_y: float32 [256], replicated, may hold values from 0.3 to 3
- symbol_z: float32 [256], replicated, may hold values from 0.3 to 3
Outputs:
- smoothed: float32 [4, 128, 256, 256], P('unit', None, 'row', 'col'), parts along dimension 0
The draws below stay inside these ranges and needn't reach their ends.
There are 2 independent parts, one for each index of `unit`. The reference program is written for one: setup_inputs(seed, part) draws one part's arguments, and reference() takes and returns one part's arrays. A program takes and returns all parts, laid end to end along the dimension named above; an argument that names none is the same for every part. Nothing has to cross between parts.
All inputs are finite; a program needn't handle non-finite values.
Results may differ from the reference program's by a relative error of at most 0.0003.
Values sent between devices are 32-bit elements.
A program may use at most 64 MiB of HBM per device.

```python
import jax
import jax.numpy as jnp
from jax import lax

GRID_X = 128
GRID_Y = 256
GRID_Z = 256
FIELDS = 2


def levels(stream_key, extent, shards, smallest, top_value):
    def one(dim, shards_of):
        steps = jax.random.uniform(jax.random.fold_in(jax.random.fold_in(stream_key, 6), dim), (shards_of,), jnp.float32, smallest / len(shards), top_value / len(shards))
        return jnp.repeat(jnp.exp(steps), extent[dim] // shards_of).reshape((-1,) + (1,) * (len(extent) - dim - 1))

    factor_of = one(*shards[0])
    for cut in shards[1:]:
        factor_of = factor_of * one(*cut)
    return factor_of


def noise(key, extent, deviation, bound, split=(), dtype=jnp.bfloat16):
    level = levels(key, extent, split, -0.22, 0.18) if split else 1.0
    drawn = jax.random.normal(key, extent, jnp.float32) * deviation * level
    return jnp.minimum(jnp.maximum(drawn, -bound), bound).astype(dtype)


def setup_inputs(seed: int = 0, part: int = 0) -> dict:
    arg_keys = jax.random.split(jax.random.key(seed), 5)
    part_keys = jax.random.split(jax.random.fold_in(arg_keys[4], part), 5)
    return {
        "tracer": noise(part_keys[0], (FIELDS, GRID_X, GRID_Y, GRID_Z), 1.0, 6.0, ((2, 16), (3, 16)), jnp.float32),
        "symbol_x": jnp.clip(jax.random.uniform(arg_keys[1], (GRID_X,), jnp.float32, 0.3, 3.0), 0.3, 3.0),
        "symbol_y": jnp.clip(jax.random.uniform(arg_keys[2], (GRID_Y,), jnp.float32, 0.3, 3.0), 0.3, 3.0),
        "symbol_z": jnp.clip(jax.random.uniform(arg_keys[3], (GRID_Z,), jnp.float32, 0.3, 3.0), 0.3, 3.0),
    }


def mode_table(count):
    rank = jnp.arange(count)
    angle = jnp.pi / (4 * count) * ((2 * rank[:, None] + 1) * (2 * rank[None, :] + 1) % (8 * count)).astype(jnp.float32)
    return jnp.cos(angle) * (2.0 / count) ** 0.5

def to_modes(values, dim):
    moved = jnp.tensordot(values, mode_table(values.shape[dim]), axes=([dim], [0]), precision=lax.Precision.HIGHEST)
    return jnp.moveaxis(moved, -1, dim)

def reference(tracer, symbol_x, symbol_y, symbol_z):
    modes = tracer
    modes = to_modes(modes, 1)
    modes = to_modes(modes, 2)
    modes = to_modes(modes, 3)
    symbol = symbol_x[:, None, None] + symbol_y[None, :, None] + symbol_z[None, None, :]
    modes = modes * lax.rsqrt(symbol)
    smoothed = modes
    smoothed = to_modes(smoothed, 3)
    smoothed = to_modes(smoothed, 2)
    smoothed = to_modes(smoothed, 1)
    return smoothed
```

```python
import functools

import jax
import jax.numpy as jnp
import numpy as np
from jax import lax
from jax.experimental import pallas as pl
from jax.experimental.pallas import tpu as pltpu
from jax.sharding import PartitionSpec as P

MESH = pl.DeviceIdType.MESH
LANES = 128
ROWS = 8
NEAR = 8


def mode_table(count):
    rank = np.arange(count)
    angle = np.pi / (4 * count) * ((2 * rank[:, None] + 1) * (2 * rank[None, :] + 1) % (8 * count))
    return np.cos(angle) * (2.0 / count) ** 0.5


def parts_of(table):
    high = table.astype(jnp.bfloat16)
    low = (table - high.astype(np.float64)).astype(jnp.bfloat16)
    return high, low


def split(values):
    high = values.astype(jnp.bfloat16)
    return high, (values - high.astype(jnp.float32)).astype(jnp.bfloat16)


def dot(a, b, dims=((1,), (0,))):
    return lax.dot_general(a, b, (dims, ((), ())), preferred_element_type=jnp.float32)


def thrice(values, axis):
    high, low = split(values)
    return jnp.concatenate([high, high, low], axis=axis)


def swap_blocks(tiles):
    count = len(tiles)
    block = LANES // count
    which = lax.broadcasted_iota(jnp.int32, tiles[0].shape, 1) // block
    tiles = list(tiles)
    bit = 1
    while bit < count:
        upper = which // bit % 2 == 1
        for i in range(count):
            if i & bit == 0:
                a, b = tiles[i], tiles[i + bit]
                tiles[i] = jnp.where(upper, pltpu.roll(b, bit * block, 1), a)
                tiles[i + bit] = jnp.where(upper, b, pltpu.roll(a, LANES - bit * block, 1))
        bit *= 2
    return tiles


def ring(count):
    return sorted(range(count), key=lambda step: -min(step, count - step))


def kernel(
    sizes, x_hbm, sx_ref, sy_hbm, sz_hbm, wx_hbm, wy_hbm, wzl_hbm, back,
    x_ref, sy_ref, sz_ref, wx_ref, wy_ref, wz_ref,
    send1, recv1, send2, recv2, send3, recv3, send4,
    load_sem, send_sem, recv_sem,
):
    fields, count_x, far_rows, cols_n = sizes
    row, col = lax.axis_index("row"), lax.axis_index("col")
    hi, me = row // NEAR, row % NEAR
    pairs = cols_n // 2
    zc, yc = col // 2, col % 2
    share = count_x // NEAR
    tall = 2 * ROWS

    near_peers = []
    for step in ring(NEAR // 2):
        for flip in (1, 0):
            if step or flip:
                near_peers.append(lax.rem(me // 2 + step, NEAR // 2) * 2 + (me + flip) % 2)
    far_peers = []
    for turn in (1, 0):
        for step in ring(pairs):
            for flip in (1, 0):
                if turn or step or flip:
                    far_peers.append(
                        ((hi + turn) % far_rows, lax.rem(zc + step, pairs) * 2 + (yc + flip) % 2)
                    )

    def near_place(peer):
        return {"row": hi * NEAR + peer, "col": col}

    def far_place(peer):
        return {"row": peer[0] * NEAR + me, "col": peer[1]}

    barrier = pltpu.get_barrier_semaphore()
    for peer in far_peers:
        pl.semaphore_signal(barrier, inc=1, device_id=far_place(peer), device_id_type=MESH)
    for peer in near_peers:
        pl.semaphore_signal(barrier, inc=1, device_id=near_place(peer), device_id_type=MESH)

    loads = [
        pltpu.make_async_copy(source, target, load_sem.at[i])
        for i, (source, target) in enumerate(
            [
                (x_hbm, x_ref),
                (wx_hbm, wx_ref),
                (sy_hbm, sy_ref),
                (sz_hbm, sz_ref),
                (wy_hbm, wy_ref),
                (wzl_hbm, wz_ref),
            ]
        )
    ]
    for load in loads:
        load.start()

    def remote(stage, source, target, where):
        return pltpu.make_async_remote_copy(
            src_ref=source,
            dst_ref=target,
            send_sem=send_sem.at[stage],
            recv_sem=recv_sem.at[stage],
            device_id=where,
            device_id_type=MESH,
        )

    loads[0].wait()
    loads[1].wait()
    modes = dot(wx_ref[...], thrice(x_ref[...], 1), ((1,), (1,)))
    for g in range(NEAR):
        for j in range(2 * fields):
            send1[g, j] = modes[g * share : (g + 1) * share, j * LANES : (j + 1) * LANES]

    pl.semaphore_wait(barrier, len(near_peers) + len(far_peers))

    mine1 = pl.ds(me * share, share)
    for peer in near_peers:
        remote(0, send1.at[peer], recv1.at[:, mine1], near_place(peer)).start()
    recv1[:, mine1] = send1[me]

    for load in loads[2:]:
        load.wait()
    count_y, count_z = sy_ref.shape[1], sz_ref.shape[1]

    def wait_stage(stage, source, target, where):
        copy = remote(stage, source, target, where)
        copy.wait_recv()

    def wait_sent(stage, source, target, where):
        remote(stage, source, target, where).wait_send()

    first = near_place(near_peers[0])
    some = far_place(far_peers[0])
    near_rest = pl.ds(0, NEAR - 1)
    far_rest = pl.ds(0, far_rows * cols_n - 1)

    copies1 = (send1.at[near_rest], send4.at[near_rest], first)
    wait_stage(0, *copies1)

    for q in range(far_rows * cols_n):
        f, k = divmod(q, share)
        for h in range(2):
            send2[q, h] = recv1[f * 2 + h, pl.ds(k, NEAR, stride=share), :]

    def slot2(ref):
        return ref.at[col, pl.ds(hi * 2, 2)]

    for peer in far_peers:
        remote(1, send2.at[peer[0] * cols_n + peer[1]], slot2(recv2), far_place(peer)).start()
    recv2[col, pl.ds(hi * 2, 2)] = send2[hi * cols_n + col]

    rank = lax.broadcasted_iota(jnp.int32, (count_y, count_y), 0)
    natural = (
        (rank // (2 * ROWS * NEAR)) * (2 * ROWS * NEAR)
        + rank % NEAR * (2 * ROWS)
        + rank // (ROWS * NEAR) % 2 * ROWS
        + rank // NEAR % ROWS
    )
    chosen = natural == lax.broadcasted_iota(jnp.int32, (count_y, count_y), 1)
    symbol_y = jnp.sum(jnp.where(chosen, sy_ref[...], 0.0), axis=1, keepdims=True)
    factor = lax.rsqrt(sx_ref[me * share + col] + symbol_y + sz_ref[...])

    copies2 = (send2.at[far_rest], recv3.at[far_rest], some)
    wait_stage(1, *copies2)

    halves = cols_n // ROWS
    tiles_t = far_rows * 2
    grid = [[None] * halves for _ in range(tiles_t * ROWS)]
    for t in range(tiles_t):
        for half in range(halves):
            tiles = [recv2[half * ROWS + i, t] for i in range(ROWS)]
            for y, tile in enumerate(swap_blocks(tiles)):
                grid[t * ROWS + y][half] = tile
    block = jnp.concatenate([jnp.concatenate(r, axis=1) for r in grid], axis=0)
    block = dot(wy_ref[...], thrice(block, 0))
    block = dot(thrice(block, 1), wz_ref[...])
    block = block * factor
    block = dot(thrice(block, 1), wz_ref[...])
    block = dot(wy_ref[...], thrice(block, 0))
    for t in range(tiles_t):
        for half in range(halves):
            tiles = [
                block[(t * ROWS + y) * NEAR : (t * ROWS + y + 1) * NEAR, half * LANES : (half + 1) * LANES]
                for y in range(ROWS)
            ]
            for i, tile in enumerate(swap_blocks(tiles)):
                send3[half * ROWS + i, t] = tile

    mine3 = hi * cols_n + col
    for peer in far_peers:
        remote(
            2, send3.at[peer[1], pl.ds(peer[0] * 2, 2)], recv3.at[mine3], far_place(peer)
        ).start()
    recv3[mine3] = send3[col, pl.ds(hi * 2, 2)]
    wait_sent(0, *copies1)
    wait_sent(1, *copies2)
    copies3 = (send2.at[far_rest], recv3.at[far_rest], some)
    wait_stage(2, *copies3)

    for s in range(NEAR):
        for f in range(fields):
            for h in range(2):
                for k in range(share // ROWS):
                    send4[s, f * 2 + h, k * ROWS : (k + 1) * ROWS] = jnp.concatenate(
                        [
                            recv3[f * share + k * ROWS + r, h, s : s + 1, :]
                            for r in range(ROWS)
                        ],
                        axis=0,
                    )
    for peer in near_peers:
        remote(3, send4.at[peer], back.at[:, mine1], near_place(peer)).start()
    back[:, mine1] = send4[me]
    copies4 = (send4.at[near_rest], send1.at[near_rest], first)
    wait_stage(3, *copies4)
    wait_sent(2, *copies3)
    wait_sent(3, *copies4)


def finish(back_ref, wx_ref, out_ref):
    for j in range(back_ref.shape[0]):
        values = thrice(back_ref[j], 0)
        out_ref[j * LANES : (j + 1) * LANES] = dot(values, wx_ref[...], ((0,), (0,)))


def fused(sizes, tracer, symbol_x, symbol_y, symbol_z):
    fields, count_x, far_rows, cols_n = sizes
    share_y, share_z = tracer.shape[2], tracer.shape[3]
    count_y, count_z = symbol_y.shape[0], symbol_z.shape[0]

    order = np.arange(count_y).reshape(far_rows, NEAR, 2, ROWS).transpose(0, 2, 3, 1).reshape(-1)
    high_x, low_x = parts_of(mode_table(count_x))
    high_y, low_y = parts_of(mode_table(count_y)[order][:, order])
    high_z, low_z = parts_of(mode_table(count_z))
    wide_x = np.concatenate([high_x, low_x, high_x], axis=1)
    tall_x = np.concatenate([high_x, low_x, high_x], axis=0)
    wide_y = np.concatenate([high_y, low_y, high_y], axis=1)
    tall_z = np.concatenate([high_z, low_z, high_z], axis=0)

    values = jnp.transpose(tracer, (0, 2, 3, 1)).reshape(fields * share_y * share_z, count_x)
    hbm = pl.BlockSpec(memory_space=pltpu.HBM)
    vmem = pl.BlockSpec(memory_space=pltpu.VMEM)
    smem = pl.BlockSpec(memory_space=pltpu.SMEM)
    operands = (
        values,
        symbol_x,
        symbol_y.reshape(1, -1),
        symbol_z.reshape(1, -1),
        jnp.asarray(wide_x),
        jnp.asarray(wide_y),
        jnp.asarray(tall_z),
    )
    held = [pltpu.VMEM(o.shape, o.dtype) for i, o in enumerate(operands) if i != 1]
    share = count_x // NEAR
    far = far_rows * cols_n

    def floats(*shape):
        return pltpu.VMEM(shape, jnp.float32)

    near_out = (NEAR, 2 * fields, share, LANES)
    back = pl.pallas_call(
        functools.partial(kernel, sizes),
        out_shape=jax.ShapeDtypeStruct((2 * fields, count_x, LANES), jnp.float32),
        in_specs=[hbm, smem] + [hbm] * 5,
        out_specs=vmem,
        scratch_shapes=held
        + [
            floats(*near_out),
            floats(2 * fields, NEAR * share, LANES),
            floats(far, 2, NEAR, LANES),
            floats(cols_n, 2 * far_rows, NEAR, LANES),
            floats(cols_n, 2 * far_rows, NEAR, LANES),
            floats(far, 2, NEAR, LANES),
            floats(*near_out),
        ]
        + [pltpu.SemaphoreType.DMA((len(held),))]
        + [pltpu.SemaphoreType.DMA((4,))] * 2,
        compiler_params=pltpu.CompilerParams(collective_id=0, has_side_effects=True),
    )(*operands)
    out = pl.pallas_call(
        finish,
        out_shape=jax.ShapeDtypeStruct(values.shape, jnp.float32),
        in_specs=[vmem, vmem],
        out_specs=vmem,
        compiler_params=pltpu.CompilerParams(),
    )(back, jnp.asarray(tall_x))
    out = out.reshape(fields, share_y, share_z, count_x)
    return jnp.transpose(out, (0, 3, 1, 2))


def to_modes(values, dim):
    table = jnp.asarray(mode_table(values.shape[dim]), jnp.float32)
    moved = jnp.tensordot(values, table, axes=([dim], [0]), precision=lax.Precision.HIGHEST)
    return jnp.moveaxis(moved, -1, dim)


def by_lines(values, symbol_x, symbol_y, symbol_z):
    values = to_modes(values, 1)
    values = lax.all_to_all(values, "row", split_axis=1, concat_axis=2, tiled=True)
    values = to_modes(values, 2)
    values = lax.all_to_all(values, "col", split_axis=2, concat_axis=3, tiled=True)
    values = to_modes(values, 3)
    share_x, share_y = values.shape[1], values.shape[2]
    part_x = lax.dynamic_slice_in_dim(symbol_x, lax.axis_index("row") * share_x, share_x)
    part_y = lax.dynamic_slice_in_dim(symbol_y, lax.axis_index("col") * share_y, share_y)
    symbol = part_x[:, None, None] + part_y[None, :, None] + symbol_z[None, None, :]
    values = values * lax.rsqrt(symbol)
    values = to_modes(values, 3)
    values = lax.all_to_all(values, "col", split_axis=3, concat_axis=2, tiled=True)
    values = to_modes(values, 2)
    values = lax.all_to_all(values, "row", split_axis=2, concat_axis=1, tiled=True)
    return to_modes(values, 1)


def solution(mesh):
    rows_n, cols_n = mesh.shape["row"], mesh.shape["col"]

    def shards(tracer, symbol_x, symbol_y, symbol_z):
        fields, count_x, share_y, share_z = tracer.shape
        fits = (
            rows_n == 2 * NEAR
            and cols_n == 2 * ROWS
            and fields == rows_n // NEAR
            and count_x == LANES
            and count_x == NEAR * cols_n
            and share_y == 2 * ROWS
            and share_z == LANES // ROWS
        )
        if not fits:
            return by_lines(tracer, symbol_x, symbol_y, symbol_z)
        sizes = fields, count_x, rows_n // NEAR, cols_n
        return fused(sizes, tracer, symbol_x, symbol_y, symbol_z)

    in_specs = (P("unit", None, "row", "col"), P(), P(), P())
    out_specs = P("unit", None, "row", "col")
    return jax.shard_map(shards, mesh=mesh, in_specs=in_specs, out_specs=out_specs, check_vma=False)
```

```python
import functools

import jax
import jax.numpy as jnp
import numpy as np
from jax import lax
from jax.experimental import pallas as pl
from jax.experimental.pallas import tpu as pltpu
from jax.sharding import PartitionSpec as P

MESH = pl.DeviceIdType.MESH
LANES = 128
ROWS = 8
NEAR = 8


def mode_table(count):
    rank = np.arange(count)
    angle = np.pi / (4 * count) * ((2 * rank[:, None] + 1) * (2 * rank[None, :] + 1) % (8 * count))
    return np.cos(angle) * (2.0 / count) ** 0.5


def parts_of(table):
    high = table.astype(jnp.bfloat16)
    low = (table - high.astype(np.float64)).astype(jnp.bfloat16)
    return high, low


def split(values):
    high = values.astype(jnp.bfloat16)
    return high, (values - high.astype(jnp.float32)).astype(jnp.bfloat16)


def dot(a, b, dims=((1,), (0,))):
    return lax.dot_general(a, b, (dims, ((), ())), preferred_element_type=jnp.float32)


def thrice(values, axis):
    high, low = split(values)
    return jnp.concatenate([high, high, low], axis=axis)


def swap_blocks(tiles):
    count = len(tiles)
    block = LANES // count
    which = lax.broadcasted_iota(jnp.int32, tiles[0].shape, 1) // block
    tiles = list(tiles)
    bit = 1
    while bit < count:
        upper = which // bit % 2 == 1
        for i in range(count):
            if i & bit == 0:
                a, b = tiles[i], tiles[i + bit]
                tiles[i] = jnp.where(upper, pltpu.roll(b, bit * block, 1), a)
                tiles[i + bit] = jnp.where(upper, b, pltpu.roll(a, LANES - bit * block, 1))
        bit *= 2
    return tiles


def ring(count):
    return sorted(range(count), key=lambda step: -min(step, count - step))


def kernel(
    sizes, x_hbm, sx_ref, sy_hbm, sz_hbm, wx_hbm, wy_hbm, wyt_hbm, wz_hbm, back,
    x_ref, sy_ref, sz_ref, wx_ref, wy_ref, wyt_ref, wz_ref,
    send1, recv1, send2, recv2, send3, recv3, send4,
    load_sem, send_sem, recv_sem,
):
    fields, count_x, far_rows, cols_n = sizes
    row, col = lax.axis_index("row"), lax.axis_index("col")
    hi, me = row >> 3, row & (NEAR - 1)
    pairs = cols_n // 2
    xc, core = me >> 1, me & 1
    zc, yc = col >> 1, col & 1
    share = count_x // NEAR

    near_peers = []
    for step in ring(NEAR // 2):
        for flip in (1, 0):
            if step or flip:
                near_peers.append(
                    ((xc + step) & (NEAR // 2 - 1)) * 2 + (1 - core if flip else core)
                )
    far_peers = []
    for turn in (1, 0):
        for step in ring(pairs):
            for flip in (1, 0):
                if turn or step or flip:
                    far_peers.append(
                        (
                            1 - hi if turn else hi,
                            ((zc + step) & (pairs - 1)) * 2 + (1 - yc if flip else yc),
                        )
                    )

    def near_place(peer):
        return {"row": hi * NEAR + peer, "col": col}

    def far_place(peer):
        return {"row": peer[0] * NEAR + me, "col": peer[1]}

    loads = [
        pltpu.make_async_copy(source, target, load_sem.at[i])
        for i, (source, target) in enumerate(
            [
                (x_hbm, x_ref),
                (wx_hbm, wx_ref),
                (sy_hbm, sy_ref),
                (sz_hbm, sz_ref),
                (wy_hbm, wy_ref),
                (wyt_hbm, wyt_ref),
                (wz_hbm, wz_ref),
            ]
        )
    ]
    for load in loads[:2]:
        load.start()

    barrier = pltpu.get_barrier_semaphore()
    for peer in far_peers:
        pl.semaphore_signal(barrier, inc=1, device_id=far_place(peer), device_id_type=MESH)
    for peer in near_peers:
        pl.semaphore_signal(barrier, inc=1, device_id=near_place(peer), device_id_type=MESH)

    def remote(stage, source, target, where):
        return pltpu.make_async_remote_copy(
            src_ref=source,
            dst_ref=target,
            send_sem=send_sem.at[stage],
            recv_sem=recv_sem.at[stage],
            device_id=where,
            device_id_type=MESH,
        )

    loads[0].wait()
    loads[1].wait()
    for load in loads[2:]:
        load.start()
    modes = dot(wx_ref[...], thrice(x_ref[...], 1), ((1,), (1,)))
    for g in range(NEAR):
        for j in range(2 * fields):
            send1[g, j] = modes[g * share : (g + 1) * share, j * LANES : (j + 1) * LANES]

    pl.semaphore_wait(barrier, len(near_peers) + len(far_peers))

    away, home = 1 - hi, hi
    halves = (away, home)
    columns = pl.ds(col * 2 * NEAR, 2 * NEAR)
    mine1 = pl.ds(me * share, share)

    def pair(half):
        return pl.ds(half * 2, 2)

    for stage, half in enumerate(halves):
        for peer in near_peers:
            remote(
                stage, send1.at[peer, pair(half)], recv1.at[pair(half), mine1], near_place(peer)
            ).start()
    recv1[:, mine1] = send1[me]

    for load in loads[2:]:
        load.wait()
    count_y, count_z = sy_ref.shape[1], sz_ref.shape[1]
    near_rest = pl.ds(0, NEAR - 1)
    one_pair = pl.ds(0, 2)
    near_copy = (
        send1.at[near_rest, one_pair],
        send4.at[near_rest, one_pair],
        near_place(near_peers[0]),
    )

    def far_copy(half):
        count = pl.ds(0, cols_n if half is away else cols_n - 1)
        return send2.at[count], send2.at[count], far_place(far_peers[0])

    away_peers = far_peers[:cols_n]
    home_peers = far_peers[cols_n:]
    for stage, (half, peers) in enumerate(zip(halves, (away_peers, home_peers))):
        remote(stage, *near_copy).wait_recv()
        for k in range(cols_n):
            for h in range(2):
                send2[half * cols_n + k, h] = recv1[half * 2 + h, pl.ds(k, NEAR, stride=share), :]
        for peer in peers:
            remote(
                2 + stage,
                send2.at[half * cols_n + peer[1]],
                recv2.at[hi, col],
                far_place(peer),
            ).start()
    recv2[hi, col] = send2[hi * cols_n + col]

    rank = lax.broadcasted_iota(jnp.int32, (count_y, count_y), 0)
    natural = (
        (rank // (2 * ROWS * NEAR)) * (2 * ROWS * NEAR)
        + rank % NEAR * (2 * ROWS)
        + rank // (ROWS * NEAR) % 2 * ROWS
        + rank // NEAR % ROWS
    )
    chosen = natural == lax.broadcasted_iota(jnp.int32, (count_y, count_y), 1)
    symbol_y = jnp.sum(jnp.where(chosen, sy_ref[...], 0.0), axis=1, keepdims=True)
    factor = lax.rsqrt(sx_ref[me * share + col] + symbol_y + sz_ref[...])

    groups = cols_n // ROWS

    def gather(half):
        rows = [[None] * groups for _ in range(2 * ROWS)]
        for h in range(2):
            for g in range(groups):
                tiles = [recv2[half, g * ROWS + i, h] for i in range(ROWS)]
                for y, tile in enumerate(swap_blocks(tiles)):
                    rows[h * ROWS + y][g] = tile
        return jnp.concatenate([jnp.concatenate(r, axis=1) for r in rows], axis=0)

    block = None
    for stage, half in ((3, home), (2, away)):
        remote(stage, *far_copy(half)).wait_recv()
        term = dot(wy_ref[half], thrice(gather(half), 0))
        block = term if block is None else block + term
    block = dot(thrice(block, 1), wz_ref[...])
    block = block * factor
    block = dot(thrice(block, 1), wz_ref[...])
    lines = thrice(block, 0)
    for stage, (half, peers) in enumerate(zip(halves, (away_peers, home_peers))):
        part = dot(wyt_ref[half], lines)
        for h in range(2):
            for g in range(groups):
                tiles = [
                    part[(h * ROWS + y) * NEAR : (h * ROWS + y + 1) * NEAR, g * LANES : (g + 1) * LANES]
                    for y in range(ROWS)
                ]
                for i, tile in enumerate(swap_blocks(tiles)):
                    send3[half, g * ROWS + i, h * NEAR : (h + 1) * NEAR] = tile
        for peer in peers:
            remote(
                4 + stage, send3.at[half, peer[1]], recv3.at[hi, columns], far_place(peer)
            ).start()
    recv3[hi, columns] = send3[hi, col]

    for stage, half in ((5, home), (4, away)):
        remote(stage, *far_copy(half)).wait_recv()
        for s in range(NEAR):
            for h in range(2):
                for k in range(cols_n // ROWS):
                    at = k * ROWS * 2 * NEAR + h * NEAR + s
                    send4[s, half * 2 + h, k * ROWS : (k + 1) * ROWS] = recv3[
                        half, pl.ds(at, ROWS, stride=2 * NEAR), :
                    ]
        for peer in near_peers:
            remote(
                2 + stage, send4.at[peer, pair(half)], back.at[pair(half), mine1], near_place(peer)
            ).start()
    back[:, mine1] = send4[me]
    for stage in (0, 1):
        remote(stage, *near_copy).wait_send()
    for stage in (2, 4):
        remote(stage, *far_copy(away)).wait_send()
    for stage in (3, 5):
        remote(stage, *far_copy(home)).wait_send()
    for stage in (7, 6):
        remote(stage, *near_copy).wait_recv()
    for stage in (7, 6):
        remote(stage, *near_copy).wait_send()


def finish(back_ref, wx_ref, out_ref):
    for j in range(back_ref.shape[0]):
        values = thrice(back_ref[j], 0)
        out_ref[j * LANES : (j + 1) * LANES] = dot(values, wx_ref[...], ((0,), (0,)))


def fused(sizes, tracer, symbol_x, symbol_y, symbol_z):
    fields, count_x, far_rows, cols_n = sizes
    share_y, share_z = tracer.shape[2], tracer.shape[3]
    count_y, count_z = symbol_y.shape[0], symbol_z.shape[0]

    order = np.arange(count_y).reshape(far_rows, NEAR, 2, ROWS).transpose(0, 2, 3, 1).reshape(-1)
    high_x, low_x = parts_of(mode_table(count_x))
    high_y, low_y = parts_of(mode_table(count_y)[order][:, order])
    high_z, low_z = parts_of(mode_table(count_z))
    wide_x = np.concatenate([high_x, low_x, high_x], axis=1)
    tall_x = np.concatenate([high_x, low_x, high_x], axis=0)
    depth = count_y // far_rows
    cuts = [slice(half * depth, (half + 1) * depth) for half in range(far_rows)]
    in_y = np.stack([np.concatenate([p[:, c] for p in (high_y, low_y, high_y)], axis=1) for c in cuts])
    out_y = np.stack([np.concatenate([p[c] for p in (high_y, low_y, high_y)], axis=1) for c in cuts])
    tall_z = np.concatenate([high_z, low_z, high_z], axis=0)

    values = jnp.transpose(tracer, (0, 2, 3, 1)).reshape(fields * share_y * share_z, count_x)
    hbm = pl.BlockSpec(memory_space=pltpu.HBM)
    vmem = pl.BlockSpec(memory_space=pltpu.VMEM)
    smem = pl.BlockSpec(memory_space=pltpu.SMEM)
    operands = (
        values,
        symbol_x,
        symbol_y.reshape(1, -1),
        symbol_z.reshape(1, -1),
        jnp.asarray(wide_x),
        jnp.asarray(in_y),
        jnp.asarray(out_y),
        jnp.asarray(tall_z),
    )
    held = [pltpu.VMEM(o.shape, o.dtype) for i, o in enumerate(operands) if i != 1]
    share = count_x // NEAR
    far = far_rows * cols_n

    def floats(*shape):
        return pltpu.VMEM(shape, jnp.float32)

    near_out = (NEAR, 2 * fields, share, LANES)
    back = pl.pallas_call(
        functools.partial(kernel, sizes),
        out_shape=pltpu.VMEM((2 * fields, count_x, LANES), jnp.float32),
        in_specs=[hbm, smem] + [hbm] * 6,
        out_specs=vmem,
        scratch_shapes=held
        + [
            floats(*near_out),
            floats(2 * fields, NEAR * share, LANES),
            floats(far, 2, NEAR, LANES),
            floats(far_rows, cols_n, 2, NEAR, LANES),
            floats(far_rows, cols_n, 2 * NEAR, LANES),
            floats(far_rows, cols_n * 2 * NEAR, LANES),
            floats(*near_out),
        ]
        + [pltpu.SemaphoreType.DMA((len(held),))]
        + [pltpu.SemaphoreType.DMA((8,))] * 2,
        compiler_params=pltpu.CompilerParams(collective_id=0, has_side_effects=True),
    )(*operands)
    out = pl.pallas_call(
        finish,
        out_shape=jax.ShapeDtypeStruct(values.shape, jnp.float32),
        in_specs=[vmem, vmem],
        out_specs=vmem,
        compiler_params=pltpu.CompilerParams(),
    )(pltpu.with_memory_space_constraint(back, pltpu.VMEM), jnp.asarray(tall_x))
    out = out.reshape(fields, share_y, share_z, count_x)
    return jnp.transpose(out, (0, 3, 1, 2))


def to_modes(values, dim):
    table = jnp.asarray(mode_table(values.shape[dim]), jnp.float32)
    moved = jnp.tensordot(values, table, axes=([dim], [0]), precision=lax.Precision.HIGHEST)
    return jnp.moveaxis(moved, -1, dim)


def by_lines(values, symbol_x, symbol_y, symbol_z):
    values = to_modes(values, 1)
    values = lax.all_to_all(values, "row", split_axis=1, concat_axis=2, tiled=True)
    values = to_modes(values, 2)
    values = lax.all_to_all(values, "col", split_axis=2, concat_axis=3, tiled=True)
    values = to_modes(values, 3)
    share_x, share_y = values.shape[1], values.shape[2]
    part_x = lax.dynamic_slice_in_dim(symbol_x, lax.axis_index("row") * share_x, share_x)
    part_y = lax.dynamic_slice_in_dim(symbol_y, lax.axis_index("col") * share_y, share_y)
    symbol = part_x[:, None, None] + part_y[None, :, None] + symbol_z[None, None, :]
    values = values * lax.rsqrt(symbol)
    values = to_modes(values, 3)
    values = lax.all_to_all(values, "col", split_axis=3, concat_axis=2, tiled=True)
    values = to_modes(values, 2)
    values = lax.all_to_all(values, "row", split_axis=2, concat_axis=1, tiled=True)
    return to_modes(values, 1)


def solution(mesh):
    rows_n, cols_n = mesh.shape["row"], mesh.shape["col"]

    def shards(tracer, symbol_x, symbol_y, symbol_z):
        fields, count_x, share_y, share_z = tracer.shape
        fits = (
            rows_n == 2 * NEAR
            and cols_n == 2 * ROWS
            and fields == rows_n // NEAR
            and count_x == LANES
            and count_x == NEAR * cols_n
            and share_y == 2 * ROWS
            and share_z == LANES // ROWS
        )
        if not fits:
            return by_lines(tracer, symbol_x, symbol_y, symbol_z)
        sizes = fields, count_x, rows_n // NEAR, cols_n
        return fused(sizes, tracer, symbol_x, symbol_y, symbol_z)

    in_specs = (P("unit", None, "row", "col"), P(), P(), P())
    out_specs = P("unit", None, "row", "col")
    return jax.shard_map(shards, mesh=mesh, in_specs=in_specs, out_specs=out_specs, check_vma=False)
```

```python
import functools

import jax
import jax.numpy as jnp
import numpy as np
from jax import lax
from jax.experimental import pallas as pl
from jax.experimental.pallas import tpu as pltpu
from jax.sharding import PartitionSpec as P

MESH = pl.DeviceIdType.MESH
LANES = 128
ROWS = 8
NEAR = 8


def mode_table(count):
    rank = np.arange(count)
    angle = np.pi / (4 * count) * ((2 * rank[:, None] + 1) * (2 * rank[None, :] + 1) % (8 * count))
    return np.cos(angle) * (2.0 / count) ** 0.5


def parts_of(table):
    high = table.astype(jnp.bfloat16)
    low = (table - high.astype(np.float64)).astype(jnp.bfloat16)
    return high, low


def split(values):
    high = values.astype(jnp.bfloat16)
    return high, (values - high.astype(jnp.float32)).astype(jnp.bfloat16)


def dot(a, b, dims=((1,), (0,))):
    return lax.dot_general(a, b, (dims, ((), ())), preferred_element_type=jnp.float32)


def thrice(values, axis):
    high, low = split(values)
    return jnp.concatenate([high, high, low], axis=axis)


def swap_blocks(tiles):
    count = len(tiles)
    block = LANES // count
    which = lax.broadcasted_iota(jnp.int32, tiles[0].shape, 1) // block
    tiles = list(tiles)
    bit = 1
    while bit < count:
        upper = which // bit % 2 == 1
        for i in range(count):
            if i & bit == 0:
                a, b = tiles[i], tiles[i + bit]
                tiles[i] = jnp.where(upper, pltpu.roll(b, bit * block, 1), a)
                tiles[i + bit] = jnp.where(upper, b, pltpu.roll(a, LANES - bit * block, 1))
        bit *= 2
    return tiles


def ring(count):
    return sorted(range(count), key=lambda step: -min(step, count - step))


def kernel(
    sizes, x_hbm, sx_ref, sy_hbm, sz_hbm, wx_hbm, wy_hbm, wyt_hbm, wz_hbm, back,
    x_ref, sy_ref, sz_ref, wx_ref, wy_ref, wyt_ref, wz_ref,
    send1, recv1, send2, recv2, send3, recv3, send4,
    load_sem, send_sem, recv_sem, near_in, far_in,
):
    fields, count_x, far_rows, cols_n = sizes
    row, col = lax.axis_index("row"), lax.axis_index("col")
    hi, me = row >> 3, row & (NEAR - 1)
    pairs = cols_n // 2
    xc, core = me >> 1, me & 1
    zc, yc = col >> 1, col & 1
    share = count_x // NEAR

    near_peers = []
    for step in ring(NEAR // 2):
        for flip in (1, 0):
            if step or flip:
                near_peers.append(
                    ((xc + step) & (NEAR // 2 - 1)) * 2 + (1 - core if flip else core)
                )
    far_peers = []
    for turn in (1, 0):
        for step in ring(pairs):
            for flip in (1, 0):
                if turn or step or flip:
                    far_peers.append(
                        (
                            1 - hi if turn else hi,
                            ((zc + step) & (pairs - 1)) * 2 + (1 - yc if flip else yc),
                        )
                    )

    def near_place(peer):
        return {"row": hi * NEAR + peer, "col": col}

    def far_place(peer):
        return {"row": peer[0] * NEAR + me, "col": peer[1]}

    loads = [
        pltpu.make_async_copy(source, target, load_sem.at[i])
        for i, (source, target) in enumerate(
            [
                (x_hbm, x_ref),
                (wx_hbm, wx_ref),
                (sy_hbm, sy_ref),
                (sz_hbm, sz_ref),
                (wy_hbm, wy_ref),
                (wyt_hbm, wyt_ref),
                (wz_hbm, wz_ref),
            ]
        )
    ]
    for load in loads[:2]:
        load.start()

    def near_key(peer):
        return (peer >> 1) * 2 + 1 - (peer & 1)

    def far_key(peer):
        return ((peer[1] >> 1) * 2 + peer[0] * 5) * 2 + (peer[1] & 1)

    near_mine, far_mine = near_key(me), far_key((hi, col))
    near_over = [near_key(peer) > near_mine for peer in near_peers]
    far_over = [far_key(peer) > far_mine for peer in far_peers]
    near_higher = sum(over.astype(jnp.int32) for over in near_over)
    far_higher = sum(over.astype(jnp.int32) for over in far_over)

    barrier = pltpu.get_barrier_semaphore()

    def tell(semaphore, where):
        pl.semaphore_signal(semaphore, inc=1, device_id=where, device_id_type=MESH)

    for peer, over in zip(far_peers, far_over):
        pl.when(over)(functools.partial(tell, barrier, far_place(peer)))
    for peer, over in zip(near_peers, near_over):
        pl.when(over)(functools.partial(tell, barrier, near_place(peer)))
    lower = len(near_peers) + len(far_peers) - near_higher - far_higher

    @pl.when(lower > 0)
    def _():
        pl.semaphore_wait(barrier, lower)

    for peer, over in zip(far_peers, far_over):
        pl.when(jnp.logical_not(over))(
            functools.partial(tell, far_in.at[hi * cols_n + col], far_place(peer))
        )
    for peer, over in zip(near_peers, near_over):
        pl.when(jnp.logical_not(over))(functools.partial(tell, near_in, near_place(peer)))

    def remote(stage, source, target, where):
        return pltpu.make_async_remote_copy(
            src_ref=source,
            dst_ref=target,
            send_sem=send_sem.at[stage],
            recv_sem=recv_sem.at[stage],
            device_id=where,
            device_id_type=MESH,
        )

    loads[0].wait()
    loads[1].wait()
    for load in loads[2:]:
        load.start()
    modes = dot(wx_ref[...], thrice(x_ref[...], 1), ((1,), (1,)))
    for g in range(NEAR):
        for j in range(2 * fields):
            send1[g, j] = modes[g * share : (g + 1) * share, j * LANES : (j + 1) * LANES]

    @pl.when(near_higher > 0)
    def _():
        pl.semaphore_wait(near_in, near_higher)

    away, home = 1 - hi, hi
    halves = (away, home)
    columns = pl.ds(col * 2 * NEAR, 2 * NEAR)
    mine1 = pl.ds(me * share, share)

    def pair(half):
        return pl.ds(half * 2, 2)

    for stage, half in enumerate(halves):
        for peer in near_peers:
            remote(
                stage, send1.at[peer, pair(half)], recv1.at[pair(half), mine1], near_place(peer)
            ).start()
    recv1[:, mine1] = send1[me]

    for load in loads[2:]:
        load.wait()
    count_y, count_z = sy_ref.shape[1], sz_ref.shape[1]
    near_rest = pl.ds(0, NEAR - 1)
    one_pair = pl.ds(0, 2)
    near_copy = (
        send1.at[near_rest, one_pair],
        send4.at[near_rest, one_pair],
        near_place(near_peers[0]),
    )

    def far_copy(half):
        count = pl.ds(0, cols_n if half is away else cols_n - 1)
        return send2.at[count], send2.at[count], far_place(far_peers[0])

    away_peers = far_peers[:cols_n]
    home_peers = far_peers[cols_n:]

    def outward(peer, stage):
        remote(
            stage, send2.at[peer[0] * cols_n + peer[1]], recv2.at[hi, col], far_place(peer)
        ).start()

    for stage, (half, first) in enumerate(zip(halves, (0, cols_n))):
        remote(stage, *near_copy).wait_recv()
        for k in range(cols_n):
            for h in range(2):
                send2[half * cols_n + k, h] = recv1[half * 2 + h, pl.ds(k, NEAR, stride=share), :]
        for peer, over in list(zip(far_peers, far_over))[first : first + cols_n]:
            pl.when(jnp.logical_not(over))(functools.partial(outward, peer, 2 + stage))

    def meet(peer):
        pl.semaphore_wait(far_in.at[peer[0] * cols_n + peer[1]], 1)
        outward(peer, 2 + (hi == peer[0]).astype(jnp.int32))

    everyone = [(a, c) for a in range(far_rows) for c in range(cols_n)]
    for peer in sorted(everyone, key=far_key):
        pl.when(far_key(peer) > far_mine)(functools.partial(meet, peer))
    recv2[hi, col] = send2[hi * cols_n + col]

    rank = lax.broadcasted_iota(jnp.int32, (count_y, count_y), 0)
    natural = (
        (rank // (2 * ROWS * NEAR)) * (2 * ROWS * NEAR)
        + rank % NEAR * (2 * ROWS)
        + rank // (ROWS * NEAR) % 2 * ROWS
        + rank // NEAR % ROWS
    )
    chosen = natural == lax.broadcasted_iota(jnp.int32, (count_y, count_y), 1)
    symbol_y = jnp.sum(jnp.where(chosen, sy_ref[...], 0.0), axis=1, keepdims=True)
    factor = lax.rsqrt(sx_ref[me * share + col] + symbol_y + sz_ref[...])

    groups = cols_n // ROWS

    def gather(half):
        rows = [[None] * groups for _ in range(2 * ROWS)]
        for h in range(2):
            for g in range(groups):
                tiles = [recv2[half, g * ROWS + i, h] for i in range(ROWS)]
                for y, tile in enumerate(swap_blocks(tiles)):
                    rows[h * ROWS + y][g] = tile
        return jnp.concatenate([jnp.concatenate(r, axis=1) for r in rows], axis=0)

    block = None
    for stage, half in ((3, home), (2, away)):
        remote(stage, *far_copy(half)).wait_recv()
        term = dot(wy_ref[half], thrice(gather(half), 0))
        block = term if block is None else block + term
    block = dot(thrice(block, 1), wz_ref[...])
    block = block * factor
    block = dot(thrice(block, 1), wz_ref[...])
    lines = thrice(block, 0)
    for stage, (half, peers) in enumerate(zip(halves, (away_peers, home_peers))):
        part = dot(wyt_ref[half], lines)
        for h in range(2):
            for g in range(groups):
                tiles = [
                    part[(h * ROWS + y) * NEAR : (h * ROWS + y + 1) * NEAR, g * LANES : (g + 1) * LANES]
                    for y in range(ROWS)
                ]
                for i, tile in enumerate(swap_blocks(tiles)):
                    send3[half, g * ROWS + i, h * NEAR : (h + 1) * NEAR] = tile
        for peer in peers:
            remote(
                4 + stage, send3.at[half, peer[1]], recv3.at[hi, columns], far_place(peer)
            ).start()
    recv3[hi, columns] = send3[hi, col]

    for stage, half in ((5, home), (4, away)):
        remote(stage, *far_copy(half)).wait_recv()
        for s in range(NEAR):
            for h in range(2):
                for k in range(cols_n // ROWS):
                    at = k * ROWS * 2 * NEAR + h * NEAR + s
                    send4[s, half * 2 + h, k * ROWS : (k + 1) * ROWS] = recv3[
                        half, pl.ds(at, ROWS, stride=2 * NEAR), :
                    ]
        for peer in near_peers:
            remote(
                2 + stage, send4.at[peer, pair(half)], back.at[pair(half), mine1], near_place(peer)
            ).start()
    back[:, mine1] = send4[me]
    for stage in (0, 1):
        remote(stage, *near_copy).wait_send()
    for stage in (2, 4):
        remote(stage, *far_copy(away)).wait_send()
    for stage in (3, 5):
        remote(stage, *far_copy(home)).wait_send()
    for stage in (7, 6):
        remote(stage, *near_copy).wait_recv()
    for stage in (7, 6):
        remote(stage, *near_copy).wait_send()


def finish(back_ref, wx_ref, out_ref):
    for j in range(back_ref.shape[0]):
        values = thrice(back_ref[j], 0)
        out_ref[j * LANES : (j + 1) * LANES] = dot(values, wx_ref[...], ((0,), (0,)))


def fused(sizes, tracer, symbol_x, symbol_y, symbol_z):
    fields, count_x, far_rows, cols_n = sizes
    share_y, share_z = tracer.shape[2], tracer.shape[3]
    count_y, count_z = symbol_y.shape[0], symbol_z.shape[0]

    order = np.arange(count_y).reshape(far_rows, NEAR, 2, ROWS).transpose(0, 2, 3, 1).reshape(-1)
    high_x, low_x = parts_of(mode_table(count_x))
    high_y, low_y = parts_of(mode_table(count_y)[order][:, order])
    high_z, low_z = parts_of(mode_table(count_z))
    wide_x = np.concatenate([high_x, low_x, high_x], axis=1)
    tall_x = np.concatenate([high_x, low_x, high_x], axis=0)
    depth = count_y // far_rows
    cuts = [slice(half * depth, (half + 1) * depth) for half in range(far_rows)]
    in_y = np.stack([np.concatenate([p[:, c] for p in (high_y, low_y, high_y)], axis=1) for c in cuts])
    out_y = np.stack([np.concatenate([p[c] for p in (high_y, low_y, high_y)], axis=1) for c in cuts])
    tall_z = np.concatenate([high_z, low_z, high_z], axis=0)

    values = jnp.transpose(tracer, (0, 2, 3, 1)).reshape(fields * share_y * share_z, count_x)
    hbm = pl.BlockSpec(memory_space=pltpu.HBM)
    vmem = pl.BlockSpec(memory_space=pltpu.VMEM)
    smem = pl.BlockSpec(memory_space=pltpu.SMEM)
    operands = (
        values,
        symbol_x,
        symbol_y.reshape(1, -1),
        symbol_z.reshape(1, -1),
        jnp.asarray(wide_x),
        jnp.asarray(in_y),
        jnp.asarray(out_y),
        jnp.asarray(tall_z),
    )
    held = [pltpu.VMEM(o.shape, o.dtype) for i, o in enumerate(operands) if i != 1]
    share = count_x // NEAR
    far = far_rows * cols_n

    def floats(*shape):
        return pltpu.VMEM(shape, jnp.float32)

    near_out = (NEAR, 2 * fields, share, LANES)
    back = pl.pallas_call(
        functools.partial(kernel, sizes),
        out_shape=pltpu.VMEM((2 * fields, count_x, LANES), jnp.float32),
        in_specs=[hbm, smem] + [hbm] * 6,
        out_specs=vmem,
        scratch_shapes=held
        + [
            floats(*near_out),
            floats(2 * fields, NEAR * share, LANES),
            floats(far, 2, NEAR, LANES),
            floats(far_rows, cols_n, 2, NEAR, LANES),
            floats(far_rows, cols_n, 2 * NEAR, LANES),
            floats(far_rows, cols_n * 2 * NEAR, LANES),
            floats(*near_out),
        ]
        + [pltpu.SemaphoreType.DMA((len(held),))]
        + [pltpu.SemaphoreType.DMA((8,))] * 2
        + [pltpu.SemaphoreType.REGULAR, pltpu.SemaphoreType.REGULAR((far,))],
        compiler_params=pltpu.CompilerParams(collective_id=0, has_side_effects=True),
    )(*operands)
    out = pl.pallas_call(
        finish,
        out_shape=jax.ShapeDtypeStruct(values.shape, jnp.float32),
        in_specs=[vmem, vmem],
        out_specs=vmem,
        compiler_params=pltpu.CompilerParams(),
    )(pltpu.with_memory_space_constraint(back, pltpu.VMEM), jnp.asarray(tall_x))
    out = out.reshape(fields, share_y, share_z, count_x)
    return jnp.transpose(out, (0, 3, 1, 2))


def to_modes(values, dim):
    table = jnp.asarray(mode_table(values.shape[dim]), jnp.float32)
    moved = jnp.tensordot(values, table, axes=([dim], [0]), precision=lax.Precision.HIGHEST)
    return jnp.moveaxis(moved, -1, dim)


def by_lines(values, symbol_x, symbol_y, symbol_z):
    values = to_modes(values, 1)
    values = lax.all_to_all(values, "row", split_axis=1, concat_axis=2, tiled=True)
    values = to_modes(values, 2)
    values = lax.all_to_all(values, "col", split_axis=2, concat_axis=3, tiled=True)
    values = to_modes(values, 3)
    share_x, share_y = values.shape[1], values.shape[2]
    part_x = lax.dynamic_slice_in_dim(symbol_x, lax.axis_index("row") * share_x, share_x)
    part_y = lax.dynamic_slice_in_dim(symbol_y, lax.axis_index("col") * share_y, share_y)
    symbol = part_x[:, None, None] + part_y[None, :, None] + symbol_z[None, None, :]
    values = values * lax.rsqrt(symbol)
    values = to_modes(values, 3)
    values = lax.all_to_all(values, "col", split_axis=3, concat_axis=2, tiled=True)
    values = to_modes(values, 2)
    values = lax.all_to_all(values, "row", split_axis=2, concat_axis=1, tiled=True)
    return to_modes(values, 1)


def solution(mesh):
    rows_n, cols_n = mesh.shape["row"], mesh.shape["col"]

    def shards(tracer, symbol_x, symbol_y, symbol_z):
        fields, count_x, share_y, share_z = tracer.shape
        fits = (
            rows_n == 2 * NEAR
            and cols_n == 2 * ROWS
            and fields == rows_n // NEAR
            and count_x == LANES
            and count_x == NEAR * cols_n
            and share_y == 2 * ROWS
            and share_z == LANES // ROWS
        )
        if not fits:
            return by_lines(tracer, symbol_x, symbol_y, symbol_z)
        sizes = fields, count_x, rows_n // NEAR, cols_n
        return fused(sizes, tracer, symbol_x, symbol_y, symbol_z)

    in_specs = (P("unit", None, "row", "col"), P(), P(), P())
    out_specs = P("unit", None, "row", "col")
    return jax.shard_map(shards, mesh=mesh, in_specs=in_specs, out_specs=out_specs, check_vma=False)
```

```python
import functools

import jax
import jax.numpy as jnp
import numpy as np
from jax import lax
from jax.experimental import pallas as pl
from jax.experimental.pallas import tpu as pltpu
from jax.sharding import PartitionSpec as P

MESH = pl.DeviceIdType.MESH
LANES = 128
ROWS = 8
NEAR = 8


def mode_table(count):
    rank = np.arange(count)
    angle = np.pi / (4 * count) * ((2 * rank[:, None] + 1) * (2 * rank[None, :] + 1) % (8 * count))
    return np.cos(angle) * (2.0 / count) ** 0.5


def parts_of(table):
    high = table.astype(jnp.bfloat16)
    low = (table - high.astype(np.float64)).astype(jnp.bfloat16)
    return high, low


def split(values):
    high = values.astype(jnp.bfloat16)
    return high, (values - high.astype(jnp.float32)).astype(jnp.bfloat16)


def dot(a, b, dims=((1,), (0,))):
    return lax.dot_general(a, b, (dims, ((), ())), preferred_element_type=jnp.float32)


def thrice(values, axis):
    high, low = split(values)
    return jnp.concatenate([high, high, low], axis=axis)


def swap_blocks(tiles):
    count = len(tiles)
    block = LANES // count
    which = lax.broadcasted_iota(jnp.int32, tiles[0].shape, 1) // block
    tiles = list(tiles)
    bit = 1
    while bit < count:
        upper = which // bit % 2 == 1
        for i in range(count):
            if i & bit == 0:
                a, b = tiles[i], tiles[i + bit]
                tiles[i] = jnp.where(upper, pltpu.roll(b, bit * block, 1), a)
                tiles[i + bit] = jnp.where(upper, b, pltpu.roll(a, LANES - bit * block, 1))
        bit *= 2
    return tiles


def ring(count):
    return sorted(range(count), key=lambda step: -min(step, count - step))


def kernel(
    sizes, x_hbm, sx_ref, sy_hbm, sz_hbm, wx_hbm, wy_hbm, wz_hbm, last_hbm,
    back_p, back_q, last_ref,
    x_ref, sy_ref, sz_ref, wx_ref, wy_ref, wz_ref,
    send_p1, recv_p1, send_q1, recv_q1, send_p2, plane, send_q2, recv_q2,
    result, recv_p3, send_q3, recv_q3, send_q4, send_p4,
    load_sem, send_sem, recv_sem,
):
    fields, count_x, far_rows, cols_n = sizes
    row, col = lax.axis_index("row"), lax.axis_index("col")
    hi, me = row >> 3, row & (NEAR - 1)
    xc, core = me >> 1, me & 1
    zc, yc = col >> 1, col & 1
    pairs, wide = cols_n // 2, NEAR // 2
    far = far_rows * cols_n
    mine = hi * cols_n + col
    in_p = core == yc
    in_q = core != yc

    near_peers = []
    for step in ring(wide):
        for flip in (1, 0):
            if step or flip:
                near_peers.append(((xc + step) & (wide - 1)) * 2 + (1 - core if flip else core))
    far_peers = []
    for turn in (1, 0):
        for step in ring(pairs):
            for flip in (1, 0):
                if turn or step or flip:
                    far_peers.append(
                        (
                            1 - hi if turn else hi,
                            ((zc + step) & (pairs - 1)) * 2 + (1 - yc if flip else yc),
                        )
                    )

    def near_place(peer):
        return {"row": hi * NEAR + peer, "col": col}

    def far_place(peer):
        return {"row": peer[0] * NEAR + me, "col": peer[1]}

    def number(peer):
        return peer[0] * cols_n + peer[1]

    loads = [
        pltpu.make_async_copy(source, target, load_sem.at[i])
        for i, (source, target) in enumerate(
            [
                (x_hbm, x_ref),
                (wx_hbm, wx_ref),
                (sy_hbm, sy_ref),
                (sz_hbm, sz_ref),
                (wy_hbm, wy_ref),
                (wz_hbm, wz_ref),
                (last_hbm, last_ref),
            ]
        )
    ]
    for load in loads[:2]:
        load.start()

    barrier = pltpu.get_barrier_semaphore()
    for peer in far_peers:
        pl.semaphore_signal(barrier, inc=1, device_id=far_place(peer), device_id_type=MESH)
    for peer in near_peers:
        pl.semaphore_signal(barrier, inc=1, device_id=near_place(peer), device_id_type=MESH)

    def remote(stage, source, target, where):
        return pltpu.make_async_remote_copy(
            src_ref=source,
            dst_ref=target,
            send_sem=send_sem.at[stage],
            recv_sem=recv_sem.at[stage],
            device_id=where,
            device_id_type=MESH,
        )

    def total(stage, ref, count):
        some = ref.at[pl.ds(0, count)]
        return remote(stage, some, some, far_place(far_peers[0]))

    def got(stage, ref, count):
        total(stage, ref, count).wait_recv()

    def sent(stage, ref, count):
        total(stage, ref, count).wait_send()

    loads[0].wait()
    loads[1].wait()
    for load in loads[2:]:
        load.start()
    modes = dot(wx_ref[...], thrice(x_ref[...], 1), ((1,), (1,)))
    middle = count_x // 2
    for f in range(fields):
        for c in range(cols_n):
            at = middle + c * wide
            send_q1[f * cols_n + c] = jnp.concatenate(
                [
                    modes[at : at + wide, (f * 2 + h) * LANES : (f * 2 + h + 1) * LANES]
                    for h in range(2)
                ],
                axis=0,
            )
    for n in range(NEAR):
        for j in range(2 * fields):
            send_p1[n, j] = modes[n * ROWS : (n + 1) * ROWS, j * LANES : (j + 1) * LANES]

    pl.semaphore_wait(barrier, len(near_peers) + len(far_peers))

    for peer in far_peers:
        remote(
            0, send_q1.at[number(peer)], recv_q1.at[pl.ds(mine * ROWS, ROWS)], far_place(peer)
        ).start()
    mine_p = pl.ds(me * ROWS, ROWS)
    for peer in near_peers:
        remote(1, send_p1.at[peer], recv_p1.at[:, mine_p], near_place(peer)).start()
    recv_p1[:, mine_p] = send_p1[me]
    recv_q1[pl.ds(mine * ROWS, ROWS)] = send_q1[mine]

    got(1, send_p1, NEAR - 1)
    for f in range(fields):
        for m in range(pairs):
            for h in range(2):
                send_p2[f * pairs + m, h] = recv_p1[f * 2 + h, pl.ds(m, NEAR, stride=ROWS), :]

    def onward_p(peer):
        return remote(
            2,
            send_p2.at[peer[0] * pairs + (peer[1] >> 1)],
            plane.at[hi, col],
            far_place(peer),
        )

    for turn in (1, 0):
        for step in ring(pairs):
            if turn or step:
                place = 1 - hi if turn else hi
                onward_p((place, ((zc + step) & (pairs - 1)) * 2 + core)).start()

    @pl.when(in_q)
    def _():
        onward_p((hi, zc * 2 + core)).start()

    @pl.when(in_p)
    def _():
        plane[hi, col] = send_p2[hi * pairs + zc]

    got(0, send_q1, far - 1)
    for w in range(wide):
        for k in range(far * 2 // ROWS):
            send_q2[w, k * ROWS : (k + 1) * ROWS] = recv_q1[
                pl.ds(k * ROWS * wide + w, ROWS, stride=wide), :
            ]
    span = far * 2
    mine_q = pl.ds(me * span, span)

    def onward_q(x, c):
        return remote(3, send_q2.at[x], recv_q2.at[mine_q], near_place(x * 2 + c))

    for step in ring(wide):
        if step:
            onward_q((xc + step) & (wide - 1), 1 - yc).start()

    @pl.when(in_p)
    def _():
        onward_q(xc, 1 - yc).start()

    @pl.when(in_q)
    def _():
        recv_q2[mine_q] = send_q2[xc]

    for load in loads[2:]:
        load.wait()
    count_y, count_z = sy_ref.shape[1], sz_ref.shape[1]
    rank = lax.broadcasted_iota(jnp.int32, (count_y, count_y), 0)
    natural = (
        (rank // (2 * ROWS * NEAR)) * (2 * ROWS * NEAR)
        + rank % NEAR * (2 * ROWS)
        + rank // (ROWS * NEAR) % 2 * ROWS
        + rank // NEAR % ROWS
    )
    chosen = natural == lax.broadcasted_iota(jnp.int32, (count_y, count_y), 1)
    symbol_y = jnp.sum(jnp.where(chosen, sy_ref[...], 0.0), axis=1, keepdims=True)
    mode = jnp.where(in_p, me * ROWS + zc, middle + col * wide + xc)
    factor = lax.rsqrt(sx_ref[mode] + symbol_y + sz_ref[...])

    @pl.when(in_p)
    def _():
        got(2, result, (far - 1) * 2 * NEAR)

    @pl.when(in_q)
    def _():
        got(3, recv_q2, (NEAR - 1) * span)
        for a in range(far_rows):
            for c in range(cols_n):
                for h in range(2):
                    at = (a * cols_n + c) * 2 + h
                    plane[a, c, h] = recv_q2[pl.ds(at, NEAR, stride=span), :]

    groups = cols_n // ROWS

    def gather(half):
        lines = [[None] * groups for _ in range(2 * ROWS)]
        for h in range(2):
            for g in range(groups):
                tiles = [plane[half, g * ROWS + i, h] for i in range(ROWS)]
                for y, tile in enumerate(swap_blocks(tiles)):
                    lines[h * ROWS + y][g] = tile
        return jnp.concatenate([jnp.concatenate(r, axis=1) for r in lines], axis=0)

    block = dot(wy_ref[...], thrice(jnp.concatenate([gather(0), gather(1)], axis=0), 0))
    block = dot(thrice(block, 1), wz_ref[...])
    block = block * factor
    block = dot(thrice(block, 1), wz_ref[...])
    block = dot(wy_ref[...], thrice(block, 0))
    for a in range(far_rows):
        for h in range(2):
            for g in range(groups):
                first = (a * 2 + h) * ROWS
                tiles = [
                    block[(first + y) * NEAR : (first + y + 1) * NEAR, g * LANES : (g + 1) * LANES]
                    for y in range(ROWS)
                ]
                for i, tile in enumerate(swap_blocks(tiles)):
                    at = (a * cols_n + g * ROWS + i) * 2 * NEAR + h * NEAR
                    result[at : at + NEAR] = tile

    tall = 2 * NEAR

    @pl.when(in_p)
    def _():
        slot = pl.ds((hi * pairs + zc) * tall, tall)
        for peer in far_peers:
            remote(
                4, result.at[pl.ds(number(peer) * tall, tall)], recv_p3.at[slot], far_place(peer)
            ).start()
        recv_p3[slot] = result[pl.ds(mine * tall, tall)]

    @pl.when(in_q)
    def _():
        for s in range(NEAR):
            for h in range(2):
                for k in range(far // ROWS):
                    at = h * far + k * ROWS
                    send_q3[s, at : at + ROWS] = result[
                        pl.ds(k * ROWS * tall + h * NEAR + s, ROWS, stride=tall), :
                    ]
        slot = pl.ds(xc * span, span)
        for peer in near_peers:
            remote(5, send_q3.at[peer], recv_q3.at[slot], near_place(peer)).start()
        recv_q3[slot] = send_q3[me]

    @pl.when(in_p)
    def _():
        got(5, recv_q2, wide * span)

    @pl.when(in_q)
    def _():
        got(5, recv_q2, (wide - 1) * span)

    for q in range(far):
        send_q4[q] = recv_q3[pl.ds(q, ROWS, stride=far), :]
    for peer in far_peers:
        remote(
            6, send_q4.at[number(peer)], back_q.at[pl.ds(mine * ROWS, ROWS)], far_place(peer)
        ).start()
    back_q[pl.ds(mine * ROWS, ROWS)] = send_q4[mine]

    @pl.when(in_p)
    def _():
        got(4, result, (far // 2 - 1) * tall)

    @pl.when(in_q)
    def _():
        got(4, result, far // 2 * tall)

    for s in range(NEAR):
        for f in range(fields):
            for h in range(2):
                send_p4[s, f * 2 + h] = recv_p3[
                    pl.ds(f * pairs * tall + h * NEAR + s, ROWS, stride=tall), :
                ]
    for peer in near_peers:
        remote(7, send_p4.at[peer], back_p.at[:, mine_p], near_place(peer)).start()
    back_p[:, mine_p] = send_p4[me]

    sent(0, send_q1, far - 1)
    sent(1, send_p1, NEAR - 1)

    @pl.when(in_p)
    def _():
        sent(2, result, (far // 2 - 1) * tall)
        sent(3, recv_q2, wide * span)
        sent(4, result, (far - 1) * tall)

    @pl.when(in_q)
    def _():
        sent(2, result, far // 2 * tall)
        sent(3, recv_q2, (wide - 1) * span)
        sent(5, recv_q2, (NEAR - 1) * span)

    got(6, send_q1, far - 1)
    got(7, send_p1, NEAR - 1)
    sent(6, send_q1, far - 1)
    sent(7, send_p1, NEAR - 1)


def finish(cols_n, back_p, back_q, table, out_hbm, held, sems):
    copies = []
    for j in range(back_p.shape[0]):
        f, h = divmod(j, 2)
        tops = [
            back_q[pl.ds((f * cols_n + c) * ROWS + h, ROWS, stride=2), :]
            for c in range(0, cols_n, 2)
        ]
        values = jnp.concatenate([back_p[j]] + tops, axis=0)
        held[j] = dot(thrice(values, 0), table[...], ((0,), (0,)))
        copy = pltpu.make_async_copy(held.at[j], out_hbm.at[pl.ds(j * LANES, LANES)], sems.at[j])
        copy.start()
        copies.append(copy)
    for copy in copies:
        copy.wait()


def fused(sizes, tracer, symbol_x, symbol_y, symbol_z):
    fields, count_x, far_rows, cols_n = sizes
    share_y, share_z = tracer.shape[2], tracer.shape[3]
    count_y, count_z = symbol_y.shape[0], symbol_z.shape[0]

    order = np.arange(count_y).reshape(far_rows, NEAR, 2, ROWS).transpose(0, 2, 3, 1).reshape(-1)
    high_x, low_x = parts_of(mode_table(count_x))
    high_y, low_y = parts_of(mode_table(count_y)[order][:, order])
    high_z, low_z = parts_of(mode_table(count_z))
    wide_x = np.concatenate([high_x, low_x, high_x], axis=1)
    tall_x = np.concatenate([high_x, low_x, high_x], axis=0)
    wide_y = np.concatenate([high_y, low_y, high_y], axis=1)
    tall_z = np.concatenate([high_z, low_z, high_z], axis=0)

    values = jnp.transpose(tracer, (0, 2, 3, 1)).reshape(fields * share_y * share_z, count_x)
    hbm = pl.BlockSpec(memory_space=pltpu.HBM)
    vmem = pl.BlockSpec(memory_space=pltpu.VMEM)
    smem = pl.BlockSpec(memory_space=pltpu.SMEM)
    operands = (
        values,
        symbol_x,
        symbol_y.reshape(1, -1),
        symbol_z.reshape(1, -1),
        jnp.asarray(wide_x),
        jnp.asarray(wide_y),
        jnp.asarray(tall_z),
        jnp.asarray(tall_x),
    )
    held = [pltpu.VMEM(o.shape, o.dtype) for i, o in enumerate(operands[:-1]) if i != 1]
    far = far_rows * cols_n

    def floats(*shape):
        return pltpu.VMEM(shape, jnp.float32)

    near_p = floats(NEAR, 2 * fields, ROWS, LANES)
    far_q = floats(far, ROWS, LANES)
    joined = floats(2 * fields, NEAR * ROWS, LANES)
    pile = floats(far * ROWS, LANES)
    handed = pl.pallas_call(
        functools.partial(kernel, sizes),
        out_shape=(joined, pile, pltpu.VMEM(tall_x.shape, jnp.bfloat16)),
        in_specs=[hbm, smem] + [hbm] * (len(operands) - 2),
        out_specs=(vmem, vmem, vmem),
        scratch_shapes=held
        + [
            near_p,
            joined,
            far_q,
            pile,
            floats(far // 2, 2, NEAR, LANES),
            floats(far_rows, cols_n, 2, NEAR, LANES),
            floats(NEAR // 2, far * 2, LANES),
            floats(NEAR * far * 2, LANES),
            floats(far * 2 * NEAR, LANES),
            floats(far * NEAR, LANES),
            floats(NEAR, far * 2, LANES),
            floats(NEAR // 2 * far * 2, LANES),
            far_q,
            near_p,
        ]
        + [pltpu.SemaphoreType.DMA((len(held) + 1,))]
        + [pltpu.SemaphoreType.DMA((8,))] * 2,
        compiler_params=pltpu.CompilerParams(collective_id=0, has_side_effects=True),
    )(*operands)
    out = pl.pallas_call(
        functools.partial(finish, cols_n),
        out_shape=jax.ShapeDtypeStruct(values.shape, jnp.float32),
        in_specs=[vmem] * 3,
        out_specs=hbm,
        scratch_shapes=[
            floats(2 * fields, LANES, LANES),
            pltpu.SemaphoreType.DMA((2 * fields,)),
        ],
    )(*[pltpu.with_memory_space_constraint(part, pltpu.VMEM) for part in handed])
    out = out.reshape(fields, share_y, share_z, count_x)
    return jnp.transpose(out, (0, 3, 1, 2))


def to_modes(values, dim):
    table = jnp.asarray(mode_table(values.shape[dim]), jnp.float32)
    moved = jnp.tensordot(values, table, axes=([dim], [0]), precision=lax.Precision.HIGHEST)
    return jnp.moveaxis(moved, -1, dim)


def by_lines(values, symbol_x, symbol_y, symbol_z):
    values = to_modes(values, 1)
    values = lax.all_to_all(values, "row", split_axis=1, concat_axis=2, tiled=True)
    values = to_modes(values, 2)
    values = lax.all_to_all(values, "col", split_axis=2, concat_axis=3, tiled=True)
    values = to_modes(values, 3)
    share_x, share_y = values.shape[1], values.shape[2]
    part_x = lax.dynamic_slice_in_dim(symbol_x, lax.axis_index("row") * share_x, share_x)
    part_y = lax.dynamic_slice_in_dim(symbol_y, lax.axis_index("col") * share_y, share_y)
    symbol = part_x[:, None, None] + part_y[None, :, None] + symbol_z[None, None, :]
    values = values * lax.rsqrt(symbol)
    values = to_modes(values, 3)
    values = lax.all_to_all(values, "col", split_axis=3, concat_axis=2, tiled=True)
    values = to_modes(values, 2)
    values = lax.all_to_all(values, "row", split_axis=2, concat_axis=1, tiled=True)
    return to_modes(values, 1)


def solution(mesh):
    rows_n, cols_n = mesh.shape["row"], mesh.shape["col"]

    def shards(tracer, symbol_x, symbol_y, symbol_z):
        fields, count_x, share_y, share_z = tracer.shape
        fits = (
            rows_n == 2 * NEAR
            and cols_n == 2 * ROWS
            and fields == rows_n // NEAR
            and count_x == LANES
            and count_x == NEAR * cols_n
            and share_y == 2 * ROWS
            and share_z == LANES // ROWS
        )
        if not fits:
            return by_lines(tracer, symbol_x, symbol_y, symbol_z)
        sizes = fields, count_x, rows_n // NEAR, cols_n
        return fused(sizes, tracer, symbol_x, symbol_y, symbol_z)

    in_specs = (P("unit", None, "row", "col"), P(), P(), P())
    out_specs = P("unit", None, "row", "col")
    return jax.shard_map(shards, mesh=mesh, in_specs=in_specs, out_specs=out_specs, check_vma=False)
```

```python
import functools

import jax
import jax.numpy as jnp
import numpy as np
from jax import lax
from jax.experimental import pallas as pl
from jax.experimental.pallas import tpu as pltpu
from jax.sharding import PartitionSpec as P

MESH = pl.DeviceIdType.MESH
LANES = 128
ROWS = 8
NEAR = 8


def mode_table(count):
    rank = np.arange(count)
    angle = np.pi / (4 * count) * ((2 * rank[:, None] + 1) * (2 * rank[None, :] + 1) % (8 * count))
    return np.cos(angle) * (2.0 / count) ** 0.5


def parts_of(table):
    high = table.astype(jnp.bfloat16)
    low = (table - high.astype(np.float64)).astype(jnp.bfloat16)
    return high, low


def split(values):
    high = values.astype(jnp.bfloat16)
    return high, (values - high.astype(jnp.float32)).astype(jnp.bfloat16)


def dot(a, b, dims=((1,), (0,))):
    return lax.dot_general(a, b, (dims, ((), ())), preferred_element_type=jnp.float32)


def thrice(values, axis):
    high, low = split(values)
    return jnp.concatenate([high, high, low], axis=axis)


def swap_blocks(tiles):
    count = len(tiles)
    block = LANES // count
    which = lax.broadcasted_iota(jnp.int32, tiles[0].shape, 1) // block
    tiles = list(tiles)
    bit = 1
    while bit < count:
        upper = which // bit % 2 == 1
        for i in range(count):
            if i & bit == 0:
                a, b = tiles[i], tiles[i + bit]
                tiles[i] = jnp.where(upper, pltpu.roll(b, bit * block, 1), a)
                tiles[i + bit] = jnp.where(upper, b, pltpu.roll(a, LANES - bit * block, 1))
        bit *= 2
    return tiles


def ring(count):
    return sorted(range(count), key=lambda step: -min(step, count - step))


def kernel(
    sizes, x_hbm, sx_hbm, sy_hbm, sz_hbm, wx_hbm, wy_hbm, wz_hbm, last_hbm,
    back_p, back_q, last_ref,
    x_ref, sx_ref, sy_ref, sz_ref, wx_ref, wy_ref, wz_ref,
    send_p1, recv_p1, send_q1, recv_q1, send_p2, plane, send_q2, recv_q2,
    result, recv_p3, send_q3, recv_q3, send_q4, send_p4,
    load_sem, send_sem, recv_sem,
):
    fields, count_x, far_rows, cols_n = sizes
    row, col = lax.axis_index("row"), lax.axis_index("col")
    hi, me = row >> 3, row & (NEAR - 1)
    xc, core = me >> 1, me & 1
    zc, yc = col >> 1, col & 1
    pairs, wide = cols_n // 2, NEAR // 2
    far = far_rows * cols_n
    mine = hi * cols_n + col
    in_p = core == yc
    in_q = core != yc

    near_peers = []
    for step in ring(wide):
        for flip in (1, 0):
            if step or flip:
                near_peers.append(((xc + step) & (wide - 1)) * 2 + (1 - core if flip else core))
    far_peers = []
    for turn in (1, 0):
        for step in ring(pairs):
            for flip in (1, 0):
                if turn or step or flip:
                    far_peers.append(
                        (
                            1 - hi if turn else hi,
                            ((zc + step) & (pairs - 1)) * 2 + (1 - yc if flip else yc),
                        )
                    )

    def near_place(peer):
        return {"row": hi * NEAR + peer, "col": col}

    def far_place(peer):
        return {"row": peer[0] * NEAR + me, "col": peer[1]}

    def number(peer):
        return peer[0] * cols_n + peer[1]

    loads = [
        pltpu.make_async_copy(source, target, load_sem.at[i])
        for i, (source, target) in enumerate(
            [
                (x_hbm, x_ref),
                (wx_hbm, wx_ref),
                (sx_hbm, sx_ref),
                (sy_hbm, sy_ref),
                (sz_hbm, sz_ref),
                (wy_hbm, wy_ref),
                (wz_hbm, wz_ref),
                (last_hbm, last_ref),
            ]
        )
    ]
    for load in loads[:2]:
        load.start()

    barrier = pltpu.get_barrier_semaphore()
    for peer in far_peers:
        pl.semaphore_signal(barrier, inc=1, device_id=far_place(peer), device_id_type=MESH)
    for peer in near_peers:
        pl.semaphore_signal(barrier, inc=1, device_id=near_place(peer), device_id_type=MESH)

    def remote(stage, source, target, where):
        return pltpu.make_async_remote_copy(
            src_ref=source,
            dst_ref=target,
            send_sem=send_sem.at[stage],
            recv_sem=recv_sem.at[stage],
            device_id=where,
            device_id_type=MESH,
        )

    def total(stage, ref, count):
        some = ref.at[pl.ds(0, count)]
        return remote(stage, some, some, far_place(far_peers[0]))

    def got(stage, ref, count):
        total(stage, ref, count).wait_recv()

    def sent(stage, ref, count):
        total(stage, ref, count).wait_send()

    loads[0].wait()
    loads[1].wait()
    for load in loads[2:]:
        load.start()
    modes = dot(wx_ref[...], thrice(x_ref[...], 1), ((1,), (1,)))
    middle = count_x // 2
    for f in range(fields):
        for c in range(cols_n):
            at = middle + c * wide
            send_q1[f * cols_n + c] = jnp.concatenate(
                [
                    modes[at : at + wide, (f * 2 + h) * LANES : (f * 2 + h + 1) * LANES]
                    for h in range(2)
                ],
                axis=0,
            )
    for n in range(NEAR):
        for j in range(2 * fields):
            send_p1[n, j] = modes[n * ROWS : (n + 1) * ROWS, j * LANES : (j + 1) * LANES]

    pl.semaphore_wait(barrier, len(near_peers) + len(far_peers))

    mine_p = pl.ds(me * ROWS, ROWS)
    for peer in near_peers:
        remote(1, send_p1.at[peer], recv_p1.at[:, mine_p], near_place(peer)).start()
    order0 = [(a, c) for a in range(far_rows) for c in range(cols_n)]
    order0.sort(key=lambda peer: (peer[1] >> 1) * 2 + peer[0] * 5)

    def first0(peer):
        remote(
            0, send_q1.at[number(peer)], recv_q1.at[pl.ds(mine * ROWS, ROWS)], far_place(peer)
        ).start()

    for peer in order0:
        pl.when(number(peer) != mine)(functools.partial(first0, peer))
    recv_p1[:, mine_p] = send_p1[me]
    recv_q1[pl.ds(mine * ROWS, ROWS)] = send_q1[mine]

    got(1, send_p1, NEAR - 1)
    for f in range(fields):
        for m in range(pairs):
            for h in range(2):
                send_p2[f * pairs + m, h] = recv_p1[f * 2 + h, pl.ds(m, NEAR, stride=ROWS), :]

    def onward_p(peer):
        return remote(
            2,
            send_p2.at[peer[0] * pairs + (peer[1] >> 1)],
            plane.at[hi, col],
            far_place(peer),
        )

    for turn in (1, 0):
        for step in ring(pairs):
            if turn or step:
                place = 1 - hi if turn else hi
                onward_p((place, ((zc + step) & (pairs - 1)) * 2 + core)).start()

    @pl.when(in_q)
    def _():
        onward_p((hi, zc * 2 + core)).start()

    @pl.when(in_p)
    def _():
        plane[hi, col] = send_p2[hi * pairs + zc]

    got(0, send_q1, far - 1)
    for w in range(wide):
        for k in range(far * 2 // ROWS):
            send_q2[w, k * ROWS : (k + 1) * ROWS] = recv_q1[
                pl.ds(k * ROWS * wide + w, ROWS, stride=wide), :
            ]
    span = far * 2
    mine_q = pl.ds(me * span, span)

    def onward_q(x, c):
        return remote(3, send_q2.at[x], recv_q2.at[mine_q], near_place(x * 2 + c))

    for step in ring(wide):
        if step:
            onward_q((xc + step) & (wide - 1), 1 - yc).start()

    @pl.when(in_p)
    def _():
        onward_q(xc, 1 - yc).start()

    @pl.when(in_q)
    def _():
        recv_q2[mine_q] = send_q2[xc]

    for load in loads[2:]:
        load.wait()
    count_y, count_z = sy_ref.shape[1], sz_ref.shape[1]
    rank = lax.broadcasted_iota(jnp.int32, (count_y, count_y), 0)
    natural = (
        (rank // (2 * ROWS * NEAR)) * (2 * ROWS * NEAR)
        + rank % NEAR * (2 * ROWS)
        + rank // (ROWS * NEAR) % 2 * ROWS
        + rank // NEAR % ROWS
    )
    chosen = natural == lax.broadcasted_iota(jnp.int32, (count_y, count_y), 1)
    symbol_y = jnp.sum(jnp.where(chosen, sy_ref[...], 0.0), axis=1, keepdims=True)
    mode = jnp.where(in_p, me * ROWS + zc, middle + col * wide + xc)
    own = lax.broadcasted_iota(jnp.int32, (1, count_x), 1) == mode
    symbol_x = jnp.sum(jnp.where(own, sx_ref[...], 0.0), axis=1, keepdims=True)
    factor = lax.rsqrt(symbol_x + symbol_y + sz_ref[...])

    @pl.when(in_p)
    def _():
        got(2, result, (far - 1) * 2 * NEAR)

    @pl.when(in_q)
    def _():
        got(3, recv_q2, (NEAR - 1) * span)
        for a in range(far_rows):
            for c in range(cols_n):
                for h in range(2):
                    at = (a * cols_n + c) * 2 + h
                    plane[a, c, h] = recv_q2[pl.ds(at, NEAR, stride=span), :]

    groups = cols_n // ROWS

    def gather(half):
        lines = [[None] * groups for _ in range(2 * ROWS)]
        for h in range(2):
            for g in range(groups):
                tiles = [plane[half, g * ROWS + i, h] for i in range(ROWS)]
                for y, tile in enumerate(swap_blocks(tiles)):
                    lines[h * ROWS + y][g] = tile
        return jnp.concatenate([jnp.concatenate(r, axis=1) for r in lines], axis=0)

    block = dot(wy_ref[...], thrice(jnp.concatenate([gather(0), gather(1)], axis=0), 0))
    block = dot(thrice(block, 1), wz_ref[...])
    block = block * factor
    block = dot(thrice(block, 1), wz_ref[...])
    block = dot(wy_ref[...], thrice(block, 0))
    for a in range(far_rows):
        for h in range(2):
            for g in range(groups):
                first = (a * 2 + h) * ROWS
                tiles = [
                    block[(first + y) * NEAR : (first + y + 1) * NEAR, g * LANES : (g + 1) * LANES]
                    for y in range(ROWS)
                ]
                for i, tile in enumerate(swap_blocks(tiles)):
                    at = (a * cols_n + g * ROWS + i) * 2 * NEAR + h * NEAR
                    result[at : at + NEAR] = tile

    tall = 2 * NEAR
    everyone = [(a, c) for a in range(far_rows) for c in range(cols_n)]
    everyone.sort(key=lambda peer: (peer[1] >> 1) * 2 + peer[0] * 5)

    def each_far(act):
        for peer in everyone:
            pl.when(number(peer) != mine)(functools.partial(act, peer))

    @pl.when(in_p)
    def _():
        slot = pl.ds((hi * pairs + zc) * tall, tall)
        def back(peer):
            remote(
                4, result.at[pl.ds(number(peer) * tall, tall)], recv_p3.at[slot], far_place(peer)
            ).start()

        each_far(back)
        recv_p3[slot] = result[pl.ds(mine * tall, tall)]

    @pl.when(in_q)
    def _():
        for s in range(NEAR):
            for h in range(2):
                for k in range(far // ROWS):
                    at = h * far + k * ROWS
                    send_q3[s, at : at + ROWS] = result[
                        pl.ds(k * ROWS * tall + h * NEAR + s, ROWS, stride=tall), :
                    ]
        slot = pl.ds(xc * span, span)
        for peer in near_peers:
            remote(5, send_q3.at[peer], recv_q3.at[slot], near_place(peer)).start()
        recv_q3[slot] = send_q3[me]

    @pl.when(in_p)
    def _():
        got(5, recv_q2, wide * span)

    @pl.when(in_q)
    def _():
        got(5, recv_q2, (wide - 1) * span)

    for q in range(far):
        send_q4[q] = recv_q3[pl.ds(q, ROWS, stride=far), :]

    def home(peer):
        remote(
            6, send_q4.at[number(peer)], back_q.at[pl.ds(mine * ROWS, ROWS)], far_place(peer)
        ).start()

    each_far(home)
    back_q[pl.ds(mine * ROWS, ROWS)] = send_q4[mine]

    @pl.when(in_p)
    def _():
        got(4, result, (far // 2 - 1) * tall)

    @pl.when(in_q)
    def _():
        got(4, result, far // 2 * tall)

    for s in range(NEAR):
        for f in range(fields):
            for h in range(2):
                send_p4[s, f * 2 + h] = recv_p3[
                    pl.ds(f * pairs * tall + h * NEAR + s, ROWS, stride=tall), :
                ]
    for peer in near_peers:
        remote(7, send_p4.at[peer], back_p.at[:, mine_p], near_place(peer)).start()
    back_p[:, mine_p] = send_p4[me]

    sent(0, send_q1, far - 1)
    sent(1, send_p1, NEAR - 1)

    @pl.when(in_p)
    def _():
        sent(2, result, (far // 2 - 1) * tall)
        sent(3, recv_q2, wide * span)
        sent(4, result, (far - 1) * tall)

    @pl.when(in_q)
    def _():
        sent(2, result, far // 2 * tall)
        sent(3, recv_q2, (wide - 1) * span)
        sent(5, recv_q2, (NEAR - 1) * span)

    got(6, send_q1, far - 1)
    got(7, send_p1, NEAR - 1)
    sent(6, send_q1, far - 1)
    sent(7, send_p1, NEAR - 1)


def finish(cols_n, back_p, back_q, table, out_hbm, held, sems):
    copies = []
    for j in range(back_p.shape[0]):
        f, h = divmod(j, 2)
        tops = [
            back_q[pl.ds((f * cols_n + c) * ROWS + h, ROWS, stride=2), :]
            for c in range(0, cols_n, 2)
        ]
        values = jnp.concatenate([back_p[j]] + tops, axis=0)
        held[j] = dot(thrice(values, 0), table[...], ((0,), (0,)))
        copy = pltpu.make_async_copy(held.at[j], out_hbm.at[pl.ds(j * LANES, LANES)], sems.at[j])
        copy.start()
        copies.append(copy)
    for copy in copies:
        copy.wait()


def fused(sizes, tracer, symbol_x, symbol_y, symbol_z):
    fields, count_x, far_rows, cols_n = sizes
    share_y, share_z = tracer.shape[2], tracer.shape[3]
    count_y, count_z = symbol_y.shape[0], symbol_z.shape[0]

    order = np.arange(count_y).reshape(far_rows, NEAR, 2, ROWS).transpose(0, 2, 3, 1).reshape(-1)
    high_x, low_x = parts_of(mode_table(count_x))
    high_y, low_y = parts_of(mode_table(count_y)[order][:, order])
    high_z, low_z = parts_of(mode_table(count_z))
    wide_x = np.concatenate([high_x, low_x, high_x], axis=1)
    tall_x = np.concatenate([high_x, low_x, high_x], axis=0)
    wide_y = np.concatenate([high_y, low_y, high_y], axis=1)
    tall_z = np.concatenate([high_z, low_z, high_z], axis=0)

    values = jnp.transpose(tracer, (0, 2, 3, 1)).reshape(fields * share_y * share_z, count_x)
    hbm = pl.BlockSpec(memory_space=pltpu.HBM)
    vmem = pl.BlockSpec(memory_space=pltpu.VMEM)
    operands = (
        values,
        symbol_x.reshape(1, -1),
        symbol_y.reshape(1, -1),
        symbol_z.reshape(1, -1),
        jnp.asarray(wide_x),
        jnp.asarray(wide_y),
        jnp.asarray(tall_z),
        jnp.asarray(tall_x),
    )
    held = [pltpu.VMEM(o.shape, o.dtype) for o in operands[:-1]]
    far = far_rows * cols_n

    def floats(*shape):
        return pltpu.VMEM(shape, jnp.float32)

    near_p = floats(NEAR, 2 * fields, ROWS, LANES)
    far_q = floats(far, ROWS, LANES)
    joined = floats(2 * fields, NEAR * ROWS, LANES)
    pile = floats(far * ROWS, LANES)
    handed = pl.pallas_call(
        functools.partial(kernel, sizes),
        out_shape=(joined, pile, pltpu.VMEM(tall_x.shape, jnp.bfloat16)),
        in_specs=[hbm] * len(operands),
        out_specs=(vmem, vmem, vmem),
        scratch_shapes=held
        + [
            near_p,
            joined,
            far_q,
            pile,
            floats(far // 2, 2, NEAR, LANES),
            floats(far_rows, cols_n, 2, NEAR, LANES),
            floats(NEAR // 2, far * 2, LANES),
            floats(NEAR * far * 2, LANES),
            floats(far * 2 * NEAR, LANES),
            floats(far * NEAR, LANES),
            floats(NEAR, far * 2, LANES),
            floats(NEAR // 2 * far * 2, LANES),
            far_q,
            near_p,
        ]
        + [pltpu.SemaphoreType.DMA((len(held) + 1,))]
        + [pltpu.SemaphoreType.DMA((8,))] * 2,
        compiler_params=pltpu.CompilerParams(collective_id=0, has_side_effects=True),
    )(*operands)
    out = pl.pallas_call(
        functools.partial(finish, cols_n),
        out_shape=jax.ShapeDtypeStruct(values.shape, jnp.float32),
        in_specs=[vmem] * 3,
        out_specs=hbm,
        scratch_shapes=[
            floats(2 * fields, LANES, LANES),
            pltpu.SemaphoreType.DMA((2 * fields,)),
        ],
    )(*[pltpu.with_memory_space_constraint(part, pltpu.VMEM) for part in handed])
    out = out.reshape(fields, share_y, share_z, count_x)
    return jnp.transpose(out, (0, 3, 1, 2))


def to_modes(values, dim):
    table = jnp.asarray(mode_table(values.shape[dim]), jnp.float32)
    moved = jnp.tensordot(values, table, axes=([dim], [0]), precision=lax.Precision.HIGHEST)
    return jnp.moveaxis(moved, -1, dim)


def by_lines(values, symbol_x, symbol_y, symbol_z):
    values = to_modes(values, 1)
    values = lax.all_to_all(values, "row", split_axis=1, concat_axis=2, tiled=True)
    values = to_modes(values, 2)
    values = lax.all_to_all(values, "col", split_axis=2, concat_axis=3, tiled=True)
    values = to_modes(values, 3)
    share_x, share_y = values.shape[1], values.shape[2]
    part_x = lax.dynamic_slice_in_dim(symbol_x, lax.axis_index("row") * share_x, share_x)
    part_y = lax.dynamic_slice_in_dim(symbol_y, lax.axis_index("col") * share_y, share_y)
    symbol = part_x[:, None, None] + part_y[None, :, None] + symbol_z[None, None, :]
    values = values * lax.rsqrt(symbol)
    values = to_modes(values, 3)
    values = lax.all_to_all(values, "col", split_axis=3, concat_axis=2, tiled=True)
    values = to_modes(values, 2)
    values = lax.all_to_all(values, "row", split_axis=2, concat_axis=1, tiled=True)
    return to_modes(values, 1)


def solution(mesh):
    rows_n, cols_n = mesh.shape["row"], mesh.shape["col"]

    def shards(tracer, symbol_x, symbol_y, symbol_z):
        fields, count_x, share_y, share_z = tracer.shape
        fits = (
            rows_n == 2 * NEAR
            and cols_n == 2 * ROWS
            and fields == rows_n // NEAR
            and count_x == LANES
            and count_x == NEAR * cols_n
            and share_y == 2 * ROWS
            and share_z == LANES // ROWS
        )
        if not fits:
            return by_lines(tracer, symbol_x, symbol_y, symbol_z)
        sizes = fields, count_x, rows_n // NEAR, cols_n
        return fused(sizes, tracer, symbol_x, symbol_y, symbol_z)

    in_specs = (P("unit", None, "row", "col"), P(), P(), P())
    out_specs = P("unit", None, "row", "col")
    return jax.shard_map(shards, mesh=mesh, in_specs=in_specs, out_specs=out_specs, check_vma=False)
```

```python
import functools

import jax
import jax.numpy as jnp
import numpy as np
from jax import lax
from jax.experimental import pallas as pl
from jax.experimental.pallas import tpu as pltpu
from jax.sharding import PartitionSpec as P

MESH = pl.DeviceIdType.MESH
LANES = 128
ROWS = 8
NEAR = 8


def mode_table(count):
    rank = np.arange(count)
    angle = np.pi / (4 * count) * ((2 * rank[:, None] + 1) * (2 * rank[None, :] + 1) % (8 * count))
    return np.cos(angle) * (2.0 / count) ** 0.5


def parts_of(table):
    high = table.astype(jnp.bfloat16)
    low = (table - high.astype(np.float64)).astype(jnp.bfloat16)
    return high, low


def split(values):
    high = values.astype(jnp.bfloat16)
    return high, (values - high.astype(jnp.float32)).astype(jnp.bfloat16)


def dot(a, b, dims=((1,), (0,))):
    return lax.dot_general(a, b, (dims, ((), ())), preferred_element_type=jnp.float32)


def thrice(values, axis):
    high, low = split(values)
    return jnp.concatenate([high, high, low], axis=axis)


def swap_blocks(tiles):
    count = len(tiles)
    block = LANES // count
    which = lax.broadcasted_iota(jnp.int32, tiles[0].shape, 1) // block
    tiles = list(tiles)
    bit = 1
    while bit < count:
        upper = which // bit % 2 == 1
        for i in range(count):
            if i & bit == 0:
                a, b = tiles[i], tiles[i + bit]
                tiles[i] = jnp.where(upper, pltpu.roll(b, bit * block, 1), a)
                tiles[i + bit] = jnp.where(upper, b, pltpu.roll(a, LANES - bit * block, 1))
        bit *= 2
    return tiles


def ring(count):
    return sorted(range(count), key=lambda step: -min(step, count - step))


def kernel(
    sizes, x_hbm, sx_hbm, sy_hbm, sz_hbm, wx_hbm, wy_hbm, wz_hbm, last_hbm,
    back_p, back_q, last_ref,
    x_ref, sx_ref, sy_ref, sz_ref, wx_ref, wy_ref, wz_ref,
    send_p1, recv_p1, send_q1, recv_q1, send_p2, plane, send_q2, recv_q2,
    result, recv_p3, send_q3, recv_q3, send_q4, send_p4,
    load_sem, send_sem, recv_sem,
):
    fields, count_x, far_rows, cols_n = sizes
    row, col = lax.axis_index("row"), lax.axis_index("col")
    hi, me = row >> 3, row & (NEAR - 1)
    xc, core = me >> 1, me & 1
    zc, yc = col >> 1, col & 1
    pairs, wide = cols_n // 2, NEAR // 2
    far = far_rows * cols_n
    mine = hi * cols_n + col
    even = zc & 1
    lane = (zc >> 1) * 2 + yc
    in_p = core == even
    in_q = core != even

    near_peers = []
    for step in ring(wide):
        for flip in (1, 0):
            if step or flip:
                near_peers.append(((xc + step) & (wide - 1)) * 2 + (1 - core if flip else core))
    far_peers = []
    for turn in (1, 0):
        for step in ring(pairs):
            for flip in (1, 0):
                if turn or step or flip:
                    far_peers.append(
                        (
                            1 - hi if turn else hi,
                            ((zc + step) & (pairs - 1)) * 2 + (1 - yc if flip else yc),
                        )
                    )

    def near_place(peer):
        return {"row": hi * NEAR + peer, "col": col}

    def far_place(peer):
        return {"row": peer[0] * NEAR + me, "col": peer[1]}

    def number(peer):
        return peer[0] * cols_n + peer[1]

    loads = [
        pltpu.make_async_copy(source, target, load_sem.at[i])
        for i, (source, target) in enumerate(
            [
                (x_hbm, x_ref),
                (wx_hbm, wx_ref),
                (sx_hbm, sx_ref),
                (sy_hbm, sy_ref),
                (sz_hbm, sz_ref),
                (wy_hbm, wy_ref),
                (wz_hbm, wz_ref),
                (last_hbm, last_ref),
            ]
        )
    ]
    for load in loads[:2]:
        load.start()

    barrier = pltpu.get_barrier_semaphore()
    for peer in far_peers:
        pl.semaphore_signal(barrier, inc=1, device_id=far_place(peer), device_id_type=MESH)
    for peer in near_peers:
        pl.semaphore_signal(barrier, inc=1, device_id=near_place(peer), device_id_type=MESH)

    def remote(stage, source, target, where):
        return pltpu.make_async_remote_copy(
            src_ref=source,
            dst_ref=target,
            send_sem=send_sem.at[stage],
            recv_sem=recv_sem.at[stage],
            device_id=where,
            device_id_type=MESH,
        )

    def total(stage, ref, count):
        some = ref.at[pl.ds(0, count)]
        return remote(stage, some, some, far_place(far_peers[0]))

    def got(stage, ref, count):
        total(stage, ref, count).wait_recv()

    def sent(stage, ref, count):
        total(stage, ref, count).wait_send()

    loads[0].wait()
    loads[1].wait()
    for load in loads[2:]:
        load.start()
    modes = dot(wx_ref[...], thrice(x_ref[...], 1), ((1,), (1,)))
    middle = count_x // 2
    for f in range(fields):
        for c in range(cols_n):
            at = middle + c * wide
            send_q1[f * cols_n + c] = jnp.concatenate(
                [
                    modes[at : at + wide, (f * 2 + h) * LANES : (f * 2 + h + 1) * LANES]
                    for h in range(2)
                ],
                axis=0,
            )
    for n in range(NEAR):
        for j in range(2 * fields):
            send_p1[n, j] = modes[n * ROWS : (n + 1) * ROWS, j * LANES : (j + 1) * LANES]

    pl.semaphore_wait(barrier, len(near_peers) + len(far_peers))

    mine_p = pl.ds(me * ROWS, ROWS)
    for peer in near_peers:
        remote(1, send_p1.at[peer], recv_p1.at[:, mine_p], near_place(peer)).start()
    order0 = [(a, c) for a in range(far_rows) for c in range(cols_n)]
    order0.sort(key=lambda peer: (peer[1] >> 1) * 2 + peer[0] * 5)

    def first0(peer):
        remote(
            0, send_q1.at[number(peer)], recv_q1.at[pl.ds(mine * ROWS, ROWS)], far_place(peer)
        ).start()

    for peer in order0:
        pl.when(number(peer) != mine)(functools.partial(first0, peer))
    recv_p1[:, mine_p] = send_p1[me]
    recv_q1[pl.ds(mine * ROWS, ROWS)] = send_q1[mine]

    got(1, send_p1, NEAR - 1)
    for f in range(fields):
        for m in range(pairs):
            for h in range(2):
                send_p2[f * pairs + m, h] = recv_p1[f * 2 + h, pl.ds(m, NEAR, stride=ROWS), :]

    def onward_p(peer):
        return remote(
            2,
            send_p2.at[peer[0] * pairs + (peer[1] >> 2) * 2 + (peer[1] & 1)],
            plane.at[hi, col],
            far_place(peer),
        )

    half = pairs // 2
    for turn in (1, 0):
        place = 1 - hi if turn else hi
        for step in ring(half):
            for flip in (1, 0):
                if turn or step or flip:
                    z = (((zc >> 1) + step) & (half - 1)) * 2 + core
                    onward_p((place, z * 2 + (1 - yc if flip else yc))).start()

    @pl.when(in_q)
    def _():
        onward_p((hi, ((zc >> 1) * 2 + core) * 2 + yc)).start()

    @pl.when(in_p)
    def _():
        plane[hi, col] = send_p2[hi * pairs + lane]

    got(0, send_q1, far - 1)
    for w in range(wide):
        for k in range(far * 2 // ROWS):
            send_q2[w, k * ROWS : (k + 1) * ROWS] = recv_q1[
                pl.ds(k * ROWS * wide + w, ROWS, stride=wide), :
            ]
    span = far * 2
    mine_q = pl.ds(me * span, span)

    def onward_q(x, c):
        return remote(3, send_q2.at[x], recv_q2.at[mine_q], near_place(x * 2 + c))

    for step in ring(wide):
        if step:
            onward_q((xc + step) & (wide - 1), 1 - even).start()

    @pl.when(in_p)
    def _():
        onward_q(xc, 1 - even).start()

    @pl.when(in_q)
    def _():
        recv_q2[mine_q] = send_q2[xc]

    for load in loads[2:]:
        load.wait()
    count_y, count_z = sy_ref.shape[1], sz_ref.shape[1]
    rank = lax.broadcasted_iota(jnp.int32, (count_y, count_y), 0)
    natural = (
        (rank // (2 * ROWS * NEAR)) * (2 * ROWS * NEAR)
        + rank % NEAR * (2 * ROWS)
        + rank // (ROWS * NEAR) % 2 * ROWS
        + rank // NEAR % ROWS
    )
    chosen = natural == lax.broadcasted_iota(jnp.int32, (count_y, count_y), 1)
    symbol_y = jnp.sum(jnp.where(chosen, sy_ref[...], 0.0), axis=1, keepdims=True)
    mode = jnp.where(in_p, me * ROWS + lane, middle + col * wide + xc)
    own = lax.broadcasted_iota(jnp.int32, (1, count_x), 1) == mode
    symbol_x = jnp.sum(jnp.where(own, sx_ref[...], 0.0), axis=1, keepdims=True)
    factor = lax.rsqrt(symbol_x + symbol_y + sz_ref[...])

    @pl.when(in_p)
    def _():
        got(2, result, (far - 1) * 2 * NEAR)

    @pl.when(in_q)
    def _():
        got(3, recv_q2, (NEAR - 1) * span)
        for a in range(far_rows):
            for c in range(cols_n):
                for h in range(2):
                    at = (a * cols_n + c) * 2 + h
                    plane[a, c, h] = recv_q2[pl.ds(at, NEAR, stride=span), :]

    groups = cols_n // ROWS

    def gather(half):
        lines = [[None] * groups for _ in range(2 * ROWS)]
        for h in range(2):
            for g in range(groups):
                tiles = [plane[half, g * ROWS + i, h] for i in range(ROWS)]
                for y, tile in enumerate(swap_blocks(tiles)):
                    lines[h * ROWS + y][g] = tile
        return jnp.concatenate([jnp.concatenate(r, axis=1) for r in lines], axis=0)

    block = dot(wy_ref[...], thrice(jnp.concatenate([gather(0), gather(1)], axis=0), 0))
    block = dot(thrice(block, 1), wz_ref[...])
    block = block * factor
    block = dot(thrice(block, 1), wz_ref[...])
    block = dot(wy_ref[...], thrice(block, 0))
    for a in range(far_rows):
        for h in range(2):
            for g in range(groups):
                first = (a * 2 + h) * ROWS
                tiles = [
                    block[(first + y) * NEAR : (first + y + 1) * NEAR, g * LANES : (g + 1) * LANES]
                    for y in range(ROWS)
                ]
                for i, tile in enumerate(swap_blocks(tiles)):
                    at = (a * cols_n + g * ROWS + i) * 2 * NEAR + h * NEAR
                    result[at : at + NEAR] = tile

    tall = 2 * NEAR
    everyone = [(a, c) for a in range(far_rows) for c in range(cols_n)]
    everyone.sort(key=lambda peer: (peer[1] >> 1) * 2 + peer[0] * 5)

    def each_far(act):
        for peer in everyone:
            pl.when(number(peer) != mine)(functools.partial(act, peer))

    @pl.when(in_p)
    def _():
        slot = pl.ds((hi * pairs + lane) * tall, tall)
        def back(peer):
            remote(
                4, result.at[pl.ds(number(peer) * tall, tall)], recv_p3.at[slot], far_place(peer)
            ).start()

        each_far(back)
        recv_p3[slot] = result[pl.ds(mine * tall, tall)]

    @pl.when(in_q)
    def _():
        for s in range(NEAR):
            for h in range(2):
                for k in range(far // ROWS):
                    at = h * far + k * ROWS
                    send_q3[s, at : at + ROWS] = result[
                        pl.ds(k * ROWS * tall + h * NEAR + s, ROWS, stride=tall), :
                    ]
        slot = pl.ds(xc * span, span)
        for peer in near_peers:
            remote(5, send_q3.at[peer], recv_q3.at[slot], near_place(peer)).start()
        recv_q3[slot] = send_q3[me]

    @pl.when(in_p)
    def _():
        got(5, recv_q2, wide * span)

    @pl.when(in_q)
    def _():
        got(5, recv_q2, (wide - 1) * span)

    for q in range(far):
        send_q4[q] = recv_q3[pl.ds(q, ROWS, stride=far), :]

    def home(peer):
        remote(
            6, send_q4.at[number(peer)], back_q.at[pl.ds(mine * ROWS, ROWS)], far_place(peer)
        ).start()

    each_far(home)
    back_q[pl.ds(mine * ROWS, ROWS)] = send_q4[mine]

    @pl.when(in_p)
    def _():
        got(4, result, (far // 2 - 1) * tall)

    @pl.when(in_q)
    def _():
        got(4, result, far // 2 * tall)

    for s in range(NEAR):
        for f in range(fields):
            for h in range(2):
                send_p4[s, f * 2 + h] = recv_p3[
                    pl.ds(f * pairs * tall + h * NEAR + s, ROWS, stride=tall), :
                ]
    for peer in near_peers:
        remote(7, send_p4.at[peer], back_p.at[:, mine_p], near_place(peer)).start()
    back_p[:, mine_p] = send_p4[me]

    sent(0, send_q1, far - 1)
    sent(1, send_p1, NEAR - 1)

    @pl.when(in_p)
    def _():
        sent(2, result, (far // 2 - 1) * tall)
        sent(3, recv_q2, wide * span)
        sent(4, result, (far - 1) * tall)

    @pl.when(in_q)
    def _():
        sent(2, result, far // 2 * tall)
        sent(3, recv_q2, (wide - 1) * span)
        sent(5, recv_q2, (NEAR - 1) * span)

    got(6, send_q1, far - 1)
    got(7, send_p1, NEAR - 1)
    sent(6, send_q1, far - 1)
    sent(7, send_p1, NEAR - 1)


def finish(cols_n, back_p, back_q, table, out_hbm, held, sems):
    copies = []
    for j in range(back_p.shape[0]):
        f, h = divmod(j, 2)
        tops = [
            back_q[pl.ds((f * cols_n + c) * ROWS + h, ROWS, stride=2), :]
            for c in range(0, cols_n, 2)
        ]
        values = jnp.concatenate([back_p[j]] + tops, axis=0)
        held[j] = dot(thrice(values, 0), table[...], ((0,), (0,)))
        copy = pltpu.make_async_copy(held.at[j], out_hbm.at[pl.ds(j * LANES, LANES)], sems.at[j])
        copy.start()
        copies.append(copy)
    for copy in copies:
        copy.wait()


def fused(sizes, tracer, symbol_x, symbol_y, symbol_z):
    fields, count_x, far_rows, cols_n = sizes
    share_y, share_z = tracer.shape[2], tracer.shape[3]
    count_y, count_z = symbol_y.shape[0], symbol_z.shape[0]

    order = np.arange(count_y).reshape(far_rows, NEAR, 2, ROWS).transpose(0, 2, 3, 1).reshape(-1)
    high_x, low_x = parts_of(mode_table(count_x))
    high_y, low_y = parts_of(mode_table(count_y)[order][:, order])
    high_z, low_z = parts_of(mode_table(count_z))
    wide_x = np.concatenate([high_x, low_x, high_x], axis=1)
    tall_x = np.concatenate([high_x, low_x, high_x], axis=0)
    wide_y = np.concatenate([high_y, low_y, high_y], axis=1)
    tall_z = np.concatenate([high_z, low_z, high_z], axis=0)

    values = jnp.transpose(tracer, (0, 2, 3, 1)).reshape(fields * share_y * share_z, count_x)
    hbm = pl.BlockSpec(memory_space=pltpu.HBM)
    vmem = pl.BlockSpec(memory_space=pltpu.VMEM)
    operands = (
        values,
        symbol_x.reshape(1, -1),
        symbol_y.reshape(1, -1),
        symbol_z.reshape(1, -1),
        jnp.asarray(wide_x),
        jnp.asarray(wide_y),
        jnp.asarray(tall_z),
        jnp.asarray(tall_x),
    )
    held = [pltpu.VMEM(o.shape, o.dtype) for o in operands[:-1]]
    far = far_rows * cols_n

    def floats(*shape):
        return pltpu.VMEM(shape, jnp.float32)

    near_p = floats(NEAR, 2 * fields, ROWS, LANES)
    far_q = floats(far, ROWS, LANES)
    joined = floats(2 * fields, NEAR * ROWS, LANES)
    pile = floats(far * ROWS, LANES)
    handed = pl.pallas_call(
        functools.partial(kernel, sizes),
        out_shape=(joined, pile, pltpu.VMEM(tall_x.shape, jnp.bfloat16)),
        in_specs=[hbm] * len(operands),
        out_specs=(vmem, vmem, vmem),
        scratch_shapes=held
        + [
            near_p,
            joined,
            far_q,
            pile,
            floats(far // 2, 2, NEAR, LANES),
            floats(far_rows, cols_n, 2, NEAR, LANES),
            floats(NEAR // 2, far * 2, LANES),
            floats(NEAR * far * 2, LANES),
            floats(far * 2 * NEAR, LANES),
            floats(far * NEAR, LANES),
            floats(NEAR, far * 2, LANES),
            floats(NEAR // 2 * far * 2, LANES),
            far_q,
            near_p,
        ]
        + [pltpu.SemaphoreType.DMA((len(held) + 1,))]
        + [pltpu.SemaphoreType.DMA((8,))] * 2,
        compiler_params=pltpu.CompilerParams(collective_id=0, has_side_effects=True),
    )(*operands)
    out = pl.pallas_call(
        functools.partial(finish, cols_n),
        out_shape=jax.ShapeDtypeStruct(values.shape, jnp.float32),
        in_specs=[vmem] * 3,
        out_specs=hbm,
        scratch_shapes=[
            floats(2 * fields, LANES, LANES),
            pltpu.SemaphoreType.DMA((2 * fields,)),
        ],
    )(*[pltpu.with_memory_space_constraint(part, pltpu.VMEM) for part in handed])
    out = out.reshape(fields, share_y, share_z, count_x)
    return jnp.transpose(out, (0, 3, 1, 2))


def to_modes(values, dim):
    table = jnp.asarray(mode_table(values.shape[dim]), jnp.float32)
    moved = jnp.tensordot(values, table, axes=([dim], [0]), precision=lax.Precision.HIGHEST)
    return jnp.moveaxis(moved, -1, dim)


def by_lines(values, symbol_x, symbol_y, symbol_z):
    values = to_modes(values, 1)
    values = lax.all_to_all(values, "row", split_axis=1, concat_axis=2, tiled=True)
    values = to_modes(values, 2)
    values = lax.all_to_all(values, "col", split_axis=2, concat_axis=3, tiled=True)
    values = to_modes(values, 3)
    share_x, share_y = values.shape[1], values.shape[2]
    part_x = lax.dynamic_slice_in_dim(symbol_x, lax.axis_index("row") * share_x, share_x)
    part_y = lax.dynamic_slice_in_dim(symbol_y, lax.axis_index("col") * share_y, share_y)
    symbol = part_x[:, None, None] + part_y[None, :, None] + symbol_z[None, None, :]
    values = values * lax.rsqrt(symbol)
    values = to_modes(values, 3)
    values = lax.all_to_all(values, "col", split_axis=3, concat_axis=2, tiled=True)
    values = to_modes(values, 2)
    values = lax.all_to_all(values, "row", split_axis=2, concat_axis=1, tiled=True)
    return to_modes(values, 1)


def solution(mesh):
    rows_n, cols_n = mesh.shape["row"], mesh.shape["col"]

    def shards(tracer, symbol_x, symbol_y, symbol_z):
        fields, count_x, share_y, share_z = tracer.shape
        fits = (
            rows_n == 2 * NEAR
            and cols_n == 2 * ROWS
            and fields == rows_n // NEAR
            and count_x == LANES
            and count_x == NEAR * cols_n
            and share_y == 2 * ROWS
            and share_z == LANES // ROWS
        )
        if not fits:
            return by_lines(tracer, symbol_x, symbol_y, symbol_z)
        sizes = fields, count_x, rows_n // NEAR, cols_n
        return fused(sizes, tracer, symbol_x, symbol_y, symbol_z)

    in_specs = (P("unit", None, "row", "col"), P(), P(), P())
    out_specs = P("unit", None, "row", "col")
    return jax.shard_map(shards, mesh=mesh, in_specs=in_specs, out_specs=out_specs, check_vma=False)
```

```python
import functools

import jax
import jax.numpy as jnp
import numpy as np
from jax import lax
from jax.experimental import pallas as pl
from jax.experimental.pallas import tpu as pltpu
from jax.sharding import PartitionSpec as P

MESH = pl.DeviceIdType.MESH
LANES = 128
ROWS = 8
NEAR = 8


def mode_table(count):
    rank = np.arange(count)
    angle = np.pi / (4 * count) * ((2 * rank[:, None] + 1) * (2 * rank[None, :] + 1) % (8 * count))
    return np.cos(angle) * (2.0 / count) ** 0.5


def parts_of(table):
    high = table.astype(jnp.bfloat16)
    low = (table - high.astype(np.float64)).astype(jnp.bfloat16)
    return high, low


def split(values):
    high = values.astype(jnp.bfloat16)
    return high, (values - high.astype(jnp.float32)).astype(jnp.bfloat16)


def dot(a, b, dims=((1,), (0,))):
    return lax.dot_general(a, b, (dims, ((), ())), preferred_element_type=jnp.float32)


def thrice(values, axis):
    high, low = split(values)
    return jnp.concatenate([high, high, low], axis=axis)


def swap_blocks(tiles):
    count = len(tiles)
    block = LANES // count
    which = lax.broadcasted_iota(jnp.int32, tiles[0].shape, 1) // block
    tiles = list(tiles)
    bit = 1
    while bit < count:
        upper = which // bit % 2 == 1
        for i in range(count):
            if i & bit == 0:
                a, b = tiles[i], tiles[i + bit]
                tiles[i] = jnp.where(upper, pltpu.roll(b, bit * block, 1), a)
                tiles[i + bit] = jnp.where(upper, b, pltpu.roll(a, LANES - bit * block, 1))
        bit *= 2
    return tiles


def ring(count):
    return sorted(range(count), key=lambda step: -min(step, count - step))


def kernel(
    sizes, x_hbm, sx_hbm, sy_hbm, sz_hbm, wx_hbm, wy_hbm, wz_hbm, last_hbm,
    back_p, back_q, last_ref,
    x_ref, sx_ref, sy_ref, sz_ref, wx_ref, wy_ref, wz_ref,
    send_p1, recv_p1, send_q1, recv_q1, send_p2, plane, send_q2, recv_q2,
    result, recv_p3, send_q3, recv_q3, send_q4, send_p4,
    load_sem, send_sem, recv_sem,
):
    fields, count_x, far_rows, cols_n = sizes
    row, col = lax.axis_index("row"), lax.axis_index("col")
    hi, me = row >> 3, row & (NEAR - 1)
    xc, core = me >> 1, me & 1
    zc, yc = col >> 1, col & 1
    pairs, wide = cols_n // 2, NEAR // 2
    far = far_rows * cols_n
    mine = hi * cols_n + col
    even = zc & 1
    lane = (zc >> 1) * 2 + yc
    in_p = core == even
    in_q = core != even

    near_peers = []
    for step in ring(wide):
        for flip in (1, 0):
            if step or flip:
                near_peers.append(((xc + step) & (wide - 1)) * 2 + (1 - core if flip else core))
    far_peers = []
    for turn in (1, 0):
        for step in ring(pairs):
            for flip in (1, 0):
                if turn or step or flip:
                    far_peers.append(
                        (
                            1 - hi if turn else hi,
                            ((zc + step) & (pairs - 1)) * 2 + (1 - yc if flip else yc),
                        )
                    )

    def near_place(peer):
        return {"row": hi * NEAR + peer, "col": col}

    def far_place(peer):
        return {"row": peer[0] * NEAR + me, "col": peer[1]}

    def number(peer):
        return peer[0] * cols_n + peer[1]

    loads = [
        pltpu.make_async_copy(source, target, load_sem.at[i])
        for i, (source, target) in enumerate(
            [
                (x_hbm, x_ref),
                (wx_hbm, wx_ref),
                (sx_hbm, sx_ref),
                (sy_hbm, sy_ref),
                (sz_hbm, sz_ref),
                (wy_hbm, wy_ref),
                (wz_hbm, wz_ref),
                (last_hbm, last_ref),
            ]
        )
    ]
    for load in loads[:2]:
        load.start()

    barrier = pltpu.get_barrier_semaphore()
    for peer in far_peers:
        pl.semaphore_signal(barrier, inc=1, device_id=far_place(peer), device_id_type=MESH)
    for peer in near_peers:
        pl.semaphore_signal(barrier, inc=1, device_id=near_place(peer), device_id_type=MESH)

    def remote(stage, source, target, where):
        return pltpu.make_async_remote_copy(
            src_ref=source,
            dst_ref=target,
            send_sem=send_sem.at[stage],
            recv_sem=recv_sem.at[stage],
            device_id=where,
            device_id_type=MESH,
        )

    def total(stage, ref, count):
        some = ref.at[pl.ds(0, count)]
        return remote(stage, some, some, far_place(far_peers[0]))

    def got(stage, ref, count):
        total(stage, ref, count).wait_recv()

    def sent(stage, ref, count):
        total(stage, ref, count).wait_send()

    loads[0].wait()
    loads[1].wait()
    for load in loads[2:]:
        load.start()
    modes = dot(wx_ref[...], thrice(x_ref[...], 1), ((1,), (1,)))
    middle = count_x // 2
    for f in range(fields):
        for c in range(cols_n):
            at = middle + c * wide
            send_q1[f * cols_n + c] = jnp.concatenate(
                [
                    modes[at : at + wide, (f * 2 + h) * LANES : (f * 2 + h + 1) * LANES]
                    for h in range(2)
                ],
                axis=0,
            )
    for n in range(NEAR):
        for j in range(2 * fields):
            send_p1[n, j] = modes[n * ROWS : (n + 1) * ROWS, j * LANES : (j + 1) * LANES]

    pl.semaphore_wait(barrier, len(near_peers) + len(far_peers))

    mine_p = pl.ds(me * ROWS, ROWS)
    for peer in near_peers:
        remote(1, send_p1.at[peer], recv_p1.at[:, mine_p], near_place(peer)).start()
    order0 = [(a, c) for a in range(far_rows) for c in range(cols_n)]
    order0.sort(key=lambda peer: (peer[1] >> 1) * 2 + peer[0] * 7)

    def first0(peer):
        remote(
            0, send_q1.at[number(peer)], recv_q1.at[pl.ds(mine * ROWS, ROWS)], far_place(peer)
        ).start()

    for peer in order0:
        pl.when(number(peer) != mine)(functools.partial(first0, peer))
    recv_p1[:, mine_p] = send_p1[me]
    recv_q1[pl.ds(mine * ROWS, ROWS)] = send_q1[mine]

    got(1, send_p1, NEAR - 1)
    for f in range(fields):
        for m in range(pairs):
            for h in range(2):
                send_p2[f * pairs + m, h] = recv_p1[f * 2 + h, pl.ds(m, NEAR, stride=ROWS), :]

    def onward_p(peer):
        return remote(
            2,
            send_p2.at[peer[0] * pairs + (peer[1] >> 2) * 2 + (peer[1] & 1)],
            plane.at[hi, col],
            far_place(peer),
        )

    half = pairs // 2
    for turn in (1, 0):
        place = 1 - hi if turn else hi
        for step in ring(half):
            for flip in (1, 0):
                if turn or step or flip:
                    z = (((zc >> 1) + step) & (half - 1)) * 2 + core
                    onward_p((place, z * 2 + (1 - yc if flip else yc))).start()

    @pl.when(in_q)
    def _():
        onward_p((hi, ((zc >> 1) * 2 + core) * 2 + yc)).start()

    @pl.when(in_p)
    def _():
        plane[hi, col] = send_p2[hi * pairs + lane]

    got(0, send_q1, far - 1)
    for w in range(wide):
        for k in range(far * 2 // ROWS):
            send_q2[w, k * ROWS : (k + 1) * ROWS] = recv_q1[
                pl.ds(k * ROWS * wide + w, ROWS, stride=wide), :
            ]
    span = far * 2
    mine_q = pl.ds(me * span, span)

    def onward_q(x, c):
        return remote(3, send_q2.at[x], recv_q2.at[mine_q], near_place(x * 2 + c))

    for step in ring(wide):
        if step:
            onward_q((xc + step) & (wide - 1), 1 - even).start()

    @pl.when(in_p)
    def _():
        onward_q(xc, 1 - even).start()

    @pl.when(in_q)
    def _():
        recv_q2[mine_q] = send_q2[xc]

    for load in loads[2:]:
        load.wait()
    count_y, count_z = sy_ref.shape[1], sz_ref.shape[1]
    rank = lax.broadcasted_iota(jnp.int32, (count_y, count_y), 0)
    natural = (
        (rank // (2 * ROWS * NEAR)) * (2 * ROWS * NEAR)
        + rank % NEAR * (2 * ROWS)
        + rank // (ROWS * NEAR) % 2 * ROWS
        + rank // NEAR % ROWS
    )
    chosen = natural == lax.broadcasted_iota(jnp.int32, (count_y, count_y), 1)
    symbol_y = jnp.sum(jnp.where(chosen, sy_ref[...], 0.0), axis=1, keepdims=True)
    mode = jnp.where(in_p, me * ROWS + lane, middle + col * wide + xc)
    own = lax.broadcasted_iota(jnp.int32, (1, count_x), 1) == mode
    symbol_x = jnp.sum(jnp.where(own, sx_ref[...], 0.0), axis=1, keepdims=True)
    factor = lax.rsqrt(symbol_x + symbol_y + sz_ref[...])

    @pl.when(in_p)
    def _():
        got(2, result, (far - 1) * 2 * NEAR)

    @pl.when(in_q)
    def _():
        got(3, recv_q2, (NEAR - 1) * span)
        for a in range(far_rows):
            for c in range(cols_n):
                for h in range(2):
                    at = (a * cols_n + c) * 2 + h
                    plane[a, c, h] = recv_q2[pl.ds(at, NEAR, stride=span), :]

    groups = cols_n // ROWS

    def gather(half):
        lines = [[None] * groups for _ in range(2 * ROWS)]
        for h in range(2):
            for g in range(groups):
                tiles = [plane[half, g * ROWS + i, h] for i in range(ROWS)]
                for y, tile in enumerate(swap_blocks(tiles)):
                    lines[h * ROWS + y][g] = tile
        return jnp.concatenate([jnp.concatenate(r, axis=1) for r in lines], axis=0)

    block = dot(wy_ref[...], thrice(jnp.concatenate([gather(0), gather(1)], axis=0), 0))
    block = dot(thrice(block, 1), wz_ref[...])
    block = block * factor
    block = dot(thrice(block, 1), wz_ref[...])
    block = dot(wy_ref[...], thrice(block, 0))
    for a in range(far_rows):
        for h in range(2):
            for g in range(groups):
                first = (a * 2 + h) * ROWS
                tiles = [
                    block[(first + y) * NEAR : (first + y + 1) * NEAR, g * LANES : (g + 1) * LANES]
                    for y in range(ROWS)
                ]
                for i, tile in enumerate(swap_blocks(tiles)):
                    at = (a * cols_n + g * ROWS + i) * 2 * NEAR + h * NEAR
                    result[at : at + NEAR] = tile

    tall = 2 * NEAR
    everyone = [(a, c) for a in range(far_rows) for c in range(cols_n)]
    everyone.sort(key=lambda peer: (peer[1] >> 1) * 2 + peer[0] * 3)

    def each_far(act):
        for peer in everyone:
            pl.when(number(peer) != mine)(functools.partial(act, peer))

    @pl.when(in_p)
    def _():
        slot = pl.ds((hi * pairs + lane) * tall, tall)
        def back(peer):
            remote(
                4, result.at[pl.ds(number(peer) * tall, tall)], recv_p3.at[slot], far_place(peer)
            ).start()

        each_far(back)
        recv_p3[slot] = result[pl.ds(mine * tall, tall)]

    @pl.when(in_q)
    def _():
        for s in range(NEAR):
            for h in range(2):
                for k in range(far // ROWS):
                    at = h * far + k * ROWS
                    send_q3[s, at : at + ROWS] = result[
                        pl.ds(k * ROWS * tall + h * NEAR + s, ROWS, stride=tall), :
                    ]
        slot = pl.ds(xc * span, span)
        for peer in near_peers:
            remote(5, send_q3.at[peer], recv_q3.at[slot], near_place(peer)).start()
        recv_q3[slot] = send_q3[me]

    @pl.when(in_p)
    def _():
        got(5, recv_q2, wide * span)

    @pl.when(in_q)
    def _():
        got(5, recv_q2, (wide - 1) * span)

    for q in range(far):
        send_q4[q] = recv_q3[pl.ds(q, ROWS, stride=far), :]

    def home(peer):
        remote(
            6, send_q4.at[number(peer)], back_q.at[pl.ds(mine * ROWS, ROWS)], far_place(peer)
        ).start()

    each_far(home)
    back_q[pl.ds(mine * ROWS, ROWS)] = send_q4[mine]

    @pl.when(in_p)
    def _():
        got(4, result, (far // 2 - 1) * tall)

    @pl.when(in_q)
    def _():
        got(4, result, far // 2 * tall)

    for s in range(NEAR):
        for f in range(fields):
            for h in range(2):
                send_p4[s, f * 2 + h] = recv_p3[
                    pl.ds(f * pairs * tall + h * NEAR + s, ROWS, stride=tall), :
                ]
    for peer in near_peers:
        remote(7, send_p4.at[peer], back_p.at[:, mine_p], near_place(peer)).start()
    back_p[:, mine_p] = send_p4[me]

    sent(0, send_q1, far - 1)
    sent(1, send_p1, NEAR - 1)

    @pl.when(in_p)
    def _():
        sent(2, result, (far // 2 - 1) * tall)
        sent(3, recv_q2, wide * span)
        sent(4, result, (far - 1) * tall)

    @pl.when(in_q)
    def _():
        sent(2, result, far // 2 * tall)
        sent(3, recv_q2, (wide - 1) * span)
        sent(5, recv_q2, (NEAR - 1) * span)

    got(6, send_q1, far - 1)
    got(7, send_p1, NEAR - 1)
    sent(6, send_q1, far - 1)
    sent(7, send_p1, NEAR - 1)


def finish(cols_n, back_p, back_q, table, out_hbm, held, sems):
    copies = []
    for j in range(back_p.shape[0]):
        f, h = divmod(j, 2)
        tops = [
            back_q[pl.ds((f * cols_n + c) * ROWS + h, ROWS, stride=2), :]
            for c in range(0, cols_n, 2)
        ]
        values = jnp.concatenate([back_p[j]] + tops, axis=0)
        held[j] = dot(thrice(values, 0), table[...], ((0,), (0,)))
        copy = pltpu.make_async_copy(held.at[j], out_hbm.at[pl.ds(j * LANES, LANES)], sems.at[j])
        copy.start()
        copies.append(copy)
    for copy in copies:
        copy.wait()


def fused(sizes, tracer, symbol_x, symbol_y, symbol_z):
    fields, count_x, far_rows, cols_n = sizes
    share_y, share_z = tracer.shape[2], tracer.shape[3]
    count_y, count_z = symbol_y.shape[0], symbol_z.shape[0]

    order = np.arange(count_y).reshape(far_rows, NEAR, 2, ROWS).transpose(0, 2, 3, 1).reshape(-1)
    high_x, low_x = parts_of(mode_table(count_x))
    high_y, low_y = parts_of(mode_table(count_y)[order][:, order])
    high_z, low_z = parts_of(mode_table(count_z))
    wide_x = np.concatenate([high_x, low_x, high_x], axis=1)
    tall_x = np.concatenate([high_x, low_x, high_x], axis=0)
    wide_y = np.concatenate([high_y, low_y, high_y], axis=1)
    tall_z = np.concatenate([high_z, low_z, high_z], axis=0)

    values = jnp.transpose(tracer, (0, 2, 3, 1)).reshape(fields * share_y * share_z, count_x)
    hbm = pl.BlockSpec(memory_space=pltpu.HBM)
    vmem = pl.BlockSpec(memory_space=pltpu.VMEM)
    operands = (
        values,
        symbol_x.reshape(1, -1),
        symbol_y.reshape(1, -1),
        symbol_z.reshape(1, -1),
        jnp.asarray(wide_x),
        jnp.asarray(wide_y),
        jnp.asarray(tall_z),
        jnp.asarray(tall_x),
    )
    held = [pltpu.VMEM(o.shape, o.dtype) for o in operands[:-1]]
    far = far_rows * cols_n

    def floats(*shape):
        return pltpu.VMEM(shape, jnp.float32)

    near_p = floats(NEAR, 2 * fields, ROWS, LANES)
    far_q = floats(far, ROWS, LANES)
    joined = floats(2 * fields, NEAR * ROWS, LANES)
    pile = floats(far * ROWS, LANES)
    handed = pl.pallas_call(
        functools.partial(kernel, sizes),
        out_shape=(joined, pile, pltpu.VMEM(tall_x.shape, jnp.bfloat16)),
        in_specs=[hbm] * len(operands),
        out_specs=(vmem, vmem, vmem),
        scratch_shapes=held
        + [
            near_p,
            joined,
            far_q,
            pile,
            floats(far // 2, 2, NEAR, LANES),
            floats(far_rows, cols_n, 2, NEAR, LANES),
            floats(NEAR // 2, far * 2, LANES),
            floats(NEAR * far * 2, LANES),
            floats(far * 2 * NEAR, LANES),
            floats(far * NEAR, LANES),
            floats(NEAR, far * 2, LANES),
            floats(NEAR // 2 * far * 2, LANES),
            far_q,
            near_p,
        ]
        + [pltpu.SemaphoreType.DMA((len(held) + 1,))]
        + [pltpu.SemaphoreType.DMA((8,))] * 2,
        compiler_params=pltpu.CompilerParams(collective_id=0, has_side_effects=True),
    )(*operands)
    out = pl.pallas_call(
        functools.partial(finish, cols_n),
        out_shape=jax.ShapeDtypeStruct(values.shape, jnp.float32),
        in_specs=[vmem] * 3,
        out_specs=hbm,
        scratch_shapes=[
            floats(2 * fields, LANES, LANES),
            pltpu.SemaphoreType.DMA((2 * fields,)),
        ],
    )(*[pltpu.with_memory_space_constraint(part, pltpu.VMEM) for part in handed])
    out = out.reshape(fields, share_y, share_z, count_x)
    return jnp.transpose(out, (0, 3, 1, 2))


def to_modes(values, dim):
    table = jnp.asarray(mode_table(values.shape[dim]), jnp.float32)
    moved = jnp.tensordot(values, table, axes=([dim], [0]), precision=lax.Precision.HIGHEST)
    return jnp.moveaxis(moved, -1, dim)


def by_lines(values, symbol_x, symbol_y, symbol_z):
    values = to_modes(values, 1)
    values = lax.all_to_all(values, "row", split_axis=1, concat_axis=2, tiled=True)
    values = to_modes(values, 2)
    values = lax.all_to_all(values, "col", split_axis=2, concat_axis=3, tiled=True)
    values = to_modes(values, 3)
    share_x, share_y = values.shape[1], values.shape[2]
    part_x = lax.dynamic_slice_in_dim(symbol_x, lax.axis_index("row") * share_x, share_x)
    part_y = lax.dynamic_slice_in_dim(symbol_y, lax.axis_index("col") * share_y, share_y)
    symbol = part_x[:, None, None] + part_y[None, :, None] + symbol_z[None, None, :]
    values = values * lax.rsqrt(symbol)
    values = to_modes(values, 3)
    values = lax.all_to_all(values, "col", split_axis=3, concat_axis=2, tiled=True)
    values = to_modes(values, 2)
    values = lax.all_to_all(values, "row", split_axis=2, concat_axis=1, tiled=True)
    return to_modes(values, 1)


def solution(mesh):
    rows_n, cols_n = mesh.shape["row"], mesh.shape["col"]

    def shards(tracer, symbol_x, symbol_y, symbol_z):
        fields, count_x, share_y, share_z = tracer.shape
        fits = (
            rows_n == 2 * NEAR
            and cols_n == 2 * ROWS
            and fields == rows_n // NEAR
            and count_x == LANES
            and count_x == NEAR * cols_n
            and share_y == 2 * ROWS
            and share_z == LANES // ROWS
        )
        if not fits:
            return by_lines(tracer, symbol_x, symbol_y, symbol_z)
        sizes = fields, count_x, rows_n // NEAR, cols_n
        return fused(sizes, tracer, symbol_x, symbol_y, symbol_z)

    in_specs = (P("unit", None, "row", "col"), P(), P(), P())
    out_specs = P("unit", None, "row", "col")
    return jax.shard_map(shards, mesh=mesh, in_specs=in_specs, out_specs=out_specs, check_vma=False)
```

```python
import functools

import jax
import jax.numpy as jnp
import numpy as np
from jax import lax
from jax.experimental import pallas as pl
from jax.experimental.pallas import tpu as pltpu
from jax.sharding import PartitionSpec as P

MESH = pl.DeviceIdType.MESH
LANES = 128
ROWS = 8
NEAR = 8


def mode_table(count):
    rank = np.arange(count)
    angle = np.pi / (4 * count) * ((2 * rank[:, None] + 1) * (2 * rank[None, :] + 1) % (8 * count))
    return np.cos(angle) * (2.0 / count) ** 0.5


def parts_of(table):
    high = table.astype(jnp.bfloat16)
    low = (table - high.astype(np.float64)).astype(jnp.bfloat16)
    return high, low


def split(values):
    high = values.astype(jnp.bfloat16)
    return high, (values - high.astype(jnp.float32)).astype(jnp.bfloat16)


def dot(a, b, dims=((1,), (0,))):
    return lax.dot_general(a, b, (dims, ((), ())), preferred_element_type=jnp.float32)


def thrice(values, axis):
    high, low = split(values)
    return jnp.concatenate([high, high, low], axis=axis)


def swap_blocks(tiles):
    count = len(tiles)
    block = LANES // count
    which = lax.broadcasted_iota(jnp.int32, tiles[0].shape, 1) // block
    tiles = list(tiles)
    bit = 1
    while bit < count:
        upper = which // bit % 2 == 1
        for i in range(count):
            if i & bit == 0:
                a, b = tiles[i], tiles[i + bit]
                tiles[i] = jnp.where(upper, pltpu.roll(b, bit * block, 1), a)
                tiles[i + bit] = jnp.where(upper, b, pltpu.roll(a, LANES - bit * block, 1))
        bit *= 2
    return tiles


def ring(count):
    return sorted(range(count), key=lambda step: -min(step, count - step))


def kernel(
    sizes, x_hbm, sx_hbm, sy_hbm, sz_hbm, wx_hbm, wy_hbm, wz_hbm, last_hbm,
    back_p, back_q, last_ref,
    x_ref, sx_ref, sy_ref, sz_ref, wx_ref, wy_ref, wz_ref,
    send_p1, recv_p1, send_q1, recv_q1, send_p2, plane, send_q2, recv_q2,
    result, recv_p3, send_q3, recv_q3, send_q4, send_p4,
    load_sem, send_sem, recv_sem,
):
    fields, count_x, far_rows, cols_n = sizes
    row, col = lax.axis_index("row"), lax.axis_index("col")
    hi, me = row >> 3, row & (NEAR - 1)
    xc, core = me >> 1, me & 1
    zc, yc = col >> 1, col & 1
    pairs, wide = cols_n // 2, NEAR // 2
    far = far_rows * cols_n
    mine = hi * cols_n + col
    even = zc & 1
    lane = (zc >> 1) * 2 + yc
    in_p = core == even
    in_q = core != even

    near_peers = []
    for step in ring(wide):
        for flip in (1, 0):
            if step or flip:
                near_peers.append(((xc + step) & (wide - 1)) * 2 + (1 - core if flip else core))
    far_peers = []
    for turn in (1, 0):
        for step in ring(pairs):
            for flip in (1, 0):
                if turn or step or flip:
                    far_peers.append(
                        (
                            1 - hi if turn else hi,
                            ((zc + step) & (pairs - 1)) * 2 + (1 - yc if flip else yc),
                        )
                    )

    def near_place(peer):
        return {"row": hi * NEAR + peer, "col": col}

    def far_place(peer):
        return {"row": peer[0] * NEAR + me, "col": peer[1]}

    def number(peer):
        return peer[0] * cols_n + peer[1]

    loads = [
        pltpu.make_async_copy(source, target, load_sem.at[i])
        for i, (source, target) in enumerate(
            [
                (x_hbm, x_ref),
                (wx_hbm, wx_ref),
                (sx_hbm, sx_ref),
                (sy_hbm, sy_ref),
                (sz_hbm, sz_ref),
                (wy_hbm, wy_ref),
                (wz_hbm, wz_ref),
                (last_hbm, last_ref),
            ]
        )
    ]
    for load in loads[:2]:
        load.start()

    barrier = pltpu.get_barrier_semaphore()
    for peer in far_peers:
        pl.semaphore_signal(barrier, inc=1, device_id=far_place(peer), device_id_type=MESH)
    for peer in near_peers:
        pl.semaphore_signal(barrier, inc=1, device_id=near_place(peer), device_id_type=MESH)

    def remote(stage, source, target, where):
        return pltpu.make_async_remote_copy(
            src_ref=source,
            dst_ref=target,
            send_sem=send_sem.at[stage],
            recv_sem=recv_sem.at[stage],
            device_id=where,
            device_id_type=MESH,
        )

    def total(stage, ref, count):
        some = ref.at[pl.ds(0, count)]
        return remote(stage, some, some, far_place(far_peers[0]))

    def got(stage, ref, count):
        total(stage, ref, count).wait_recv()

    def sent(stage, ref, count):
        total(stage, ref, count).wait_send()

    loads[0].wait()
    loads[1].wait()
    for load in loads[2:]:
        load.start()
    modes = dot(wx_ref[...], thrice(x_ref[...], 1), ((1,), (1,)))
    middle = count_x // 2
    for f in range(fields):
        for c in range(cols_n):
            at = middle + c * wide
            send_q1[f * cols_n + c] = jnp.concatenate(
                [
                    modes[at : at + wide, (f * 2 + h) * LANES : (f * 2 + h + 1) * LANES]
                    for h in range(2)
                ],
                axis=0,
            )
    for n in range(NEAR):
        for j in range(2 * fields):
            send_p1[n, j] = modes[n * ROWS : (n + 1) * ROWS, j * LANES : (j + 1) * LANES]

    pl.semaphore_wait(barrier, len(near_peers) + len(far_peers))

    mine_p = pl.ds(me * ROWS, ROWS)
    for peer in near_peers:
        remote(1, send_p1.at[peer], recv_p1.at[:, mine_p], near_place(peer)).start()
    order0 = [(a, c) for a in range(far_rows) for c in range(cols_n)]
    order0.sort(key=lambda peer: (peer[1] >> 1) * 2 + peer[0] * 7)

    def first0(peer):
        remote(
            0, send_q1.at[number(peer)], recv_q1.at[pl.ds(mine * ROWS, ROWS)], far_place(peer)
        ).start()

    for peer in order0:
        pl.when(number(peer) != mine)(functools.partial(first0, peer))
    recv_p1[:, mine_p] = send_p1[me]
    recv_q1[pl.ds(mine * ROWS, ROWS)] = send_q1[mine]

    got(1, send_p1, NEAR - 1)
    for f in range(fields):
        for m in range(pairs):
            for h in range(2):
                send_p2[f * pairs + m, h] = recv_p1[f * 2 + h, pl.ds(m, NEAR, stride=ROWS), :]

    def onward_p(peer):
        return remote(
            2,
            send_p2.at[peer[0] * pairs + (peer[1] >> 2) * 2 + (peer[1] & 1)],
            plane.at[hi, col],
            far_place(peer),
        )

    half = pairs // 2
    for turn in (1, 0):
        place = 1 - hi if turn else hi
        for step in ring(half):
            for flip in (1, 0):
                if turn or step or flip:
                    z = (((zc >> 1) + step) & (half - 1)) * 2 + core
                    onward_p((place, z * 2 + (1 - yc if flip else yc))).start()

    @pl.when(in_q)
    def _():
        onward_p((hi, ((zc >> 1) * 2 + core) * 2 + yc)).start()

    @pl.when(in_p)
    def _():
        plane[hi, col] = send_p2[hi * pairs + lane]

    got(0, send_q1, far - 1)
    for w in range(wide):
        for k in range(far * 2 // ROWS):
            send_q2[w, k * ROWS : (k + 1) * ROWS] = recv_q1[
                pl.ds(k * ROWS * wide + w, ROWS, stride=wide), :
            ]
    span = far * 2
    mine_q = pl.ds(me * span, span)

    def onward_q(x, c):
        return remote(3, send_q2.at[x], recv_q2.at[mine_q], near_place(x * 2 + c))

    for step in ring(wide):
        if step:
            onward_q((xc + step) & (wide - 1), 1 - even).start()

    @pl.when(in_p)
    def _():
        onward_q(xc, 1 - even).start()

    @pl.when(in_q)
    def _():
        recv_q2[mine_q] = send_q2[xc]

    for load in loads[2:]:
        load.wait()
    count_y, count_z = sy_ref.shape[1], sz_ref.shape[1]
    rank = lax.broadcasted_iota(jnp.int32, (count_y, count_y), 0)
    natural = (
        (rank // (2 * ROWS * NEAR)) * (2 * ROWS * NEAR)
        + rank % NEAR * (2 * ROWS)
        + rank // (ROWS * NEAR) % 2 * ROWS
        + rank // NEAR % ROWS
    )
    chosen = natural == lax.broadcasted_iota(jnp.int32, (count_y, count_y), 1)
    symbol_y = jnp.sum(jnp.where(chosen, sy_ref[...], 0.0), axis=1, keepdims=True)
    mode = jnp.where(in_p, me * ROWS + lane, middle + col * wide + xc)
    own = lax.broadcasted_iota(jnp.int32, (1, count_x), 1) == mode
    symbol_x = jnp.sum(jnp.where(own, sx_ref[...], 0.0), axis=1, keepdims=True)
    factor = lax.rsqrt(symbol_x + symbol_y + sz_ref[...])

    @pl.when(in_p)
    def _():
        got(2, result, (far - 1) * 2 * NEAR)

    @pl.when(in_q)
    def _():
        got(3, recv_q2, (NEAR - 1) * span)
        for a in range(far_rows):
            for c in range(cols_n):
                for h in range(2):
                    at = (a * cols_n + c) * 2 + h
                    plane[a, c, h] = recv_q2[pl.ds(at, NEAR, stride=span), :]

    groups = cols_n // ROWS

    def gather(half):
        lines = [[None] * groups for _ in range(2 * ROWS)]
        for h in range(2):
            for g in range(groups):
                tiles = [plane[half, g * ROWS + i, h] for i in range(ROWS)]
                for y, tile in enumerate(swap_blocks(tiles)):
                    lines[h * ROWS + y][g] = tile
        return jnp.concatenate([jnp.concatenate(r, axis=1) for r in lines], axis=0)

    block = dot(wy_ref[...], thrice(jnp.concatenate([gather(0), gather(1)], axis=0), 0))
    block = dot(thrice(block, 1), wz_ref[...])
    block = block * factor
    block = dot(thrice(block, 1), wz_ref[...])
    block = dot(wy_ref[...], thrice(block, 0))
    for a in range(far_rows):
        for h in range(2):
            for g in range(groups):
                first = (a * 2 + h) * ROWS
                tiles = [
                    block[(first + y) * NEAR : (first + y + 1) * NEAR, g * LANES : (g + 1) * LANES]
                    for y in range(ROWS)
                ]
                for i, tile in enumerate(swap_blocks(tiles)):
                    at = (a * cols_n + g * ROWS + i) * 2 * NEAR + h * NEAR
                    result[at : at + NEAR] = tile

    tall = 2 * NEAR
    everyone = [(a, c) for a in range(far_rows) for c in range(cols_n)]
    everyone.sort(key=lambda peer: (peer[1] >> 1) * 2 + peer[0] * 3)

    def each_far(act):
        for peer in everyone:
            pl.when(number(peer) != mine)(functools.partial(act, peer))

    @pl.when(in_q)
    def _():
        for s in range(NEAR):
            for h in range(2):
                for k in range(far // ROWS):
                    at = h * far + k * ROWS
                    send_q3[s, at : at + ROWS] = result[
                        pl.ds(k * ROWS * tall + h * NEAR + s, ROWS, stride=tall), :
                    ]
        slot = pl.ds(xc * span, span)
        for peer in near_peers:
            remote(5, send_q3.at[peer], recv_q3.at[slot], near_place(peer)).start()
        recv_q3[slot] = send_q3[me]

    @pl.when(in_p)
    def _():
        slot = pl.ds((hi * pairs + lane) * tall, tall)
        def back(peer):
            remote(
                4, result.at[pl.ds(number(peer) * tall, tall)], recv_p3.at[slot], far_place(peer)
            ).start()

        each_far(back)
        recv_p3[slot] = result[pl.ds(mine * tall, tall)]

    @pl.when(in_p)
    def _():
        got(5, recv_q2, wide * span)

    @pl.when(in_q)
    def _():
        got(5, recv_q2, (wide - 1) * span)

    for q in range(far):
        send_q4[q] = recv_q3[pl.ds(q, ROWS, stride=far), :]

    def home(peer):
        remote(
            6, send_q4.at[number(peer)], back_q.at[pl.ds(mine * ROWS, ROWS)], far_place(peer)
        ).start()

    each_far(home)
    back_q[pl.ds(mine * ROWS, ROWS)] = send_q4[mine]

    @pl.when(in_p)
    def _():
        got(4, result, (far // 2 - 1) * tall)

    @pl.when(in_q)
    def _():
        got(4, result, far // 2 * tall)

    for s in range(NEAR):
        for f in range(fields):
            for h in range(2):
                send_p4[s, f * 2 + h] = recv_p3[
                    pl.ds(f * pairs * tall + h * NEAR + s, ROWS, stride=tall), :
                ]
    for peer in near_peers:
        remote(7, send_p4.at[peer], back_p.at[:, mine_p], near_place(peer)).start()
    back_p[:, mine_p] = send_p4[me]

    sent(0, send_q1, far - 1)
    sent(1, send_p1, NEAR - 1)

    @pl.when(in_p)
    def _():
        sent(2, result, (far // 2 - 1) * tall)
        sent(3, recv_q2, wide * span)
        sent(4, result, (far - 1) * tall)

    @pl.when(in_q)
    def _():
        sent(2, result, far // 2 * tall)
        sent(3, recv_q2, (wide - 1) * span)
        sent(5, recv_q2, (NEAR - 1) * span)

    got(6, send_q1, far - 1)
    got(7, send_p1, NEAR - 1)
    sent(6, send_q1, far - 1)
    sent(7, send_p1, NEAR - 1)


def finish(cols_n, back_p, back_q, table, out_hbm, held, sems):
    copies = []
    for j in range(back_p.shape[0]):
        f, h = divmod(j, 2)
        tops = [
            back_q[pl.ds((f * cols_n + c) * ROWS + h, ROWS, stride=2), :]
            for c in range(0, cols_n, 2)
        ]
        values = jnp.concatenate([back_p[j]] + tops, axis=0)
        held[j] = dot(thrice(values, 0), table[...], ((0,), (0,)))
        copy = pltpu.make_async_copy(held.at[j], out_hbm.at[pl.ds(j * LANES, LANES)], sems.at[j])
        copy.start()
        copies.append(copy)
    for copy in copies:
        copy.wait()


def fused(sizes, tracer, symbol_x, symbol_y, symbol_z):
    fields, count_x, far_rows, cols_n = sizes
    share_y, share_z = tracer.shape[2], tracer.shape[3]
    count_y, count_z = symbol_y.shape[0], symbol_z.shape[0]

    order = np.arange(count_y).reshape(far_rows, NEAR, 2, ROWS).transpose(0, 2, 3, 1).reshape(-1)
    high_x, low_x = parts_of(mode_table(count_x))
    high_y, low_y = parts_of(mode_table(count_y)[order][:, order])
    high_z, low_z = parts_of(mode_table(count_z))
    wide_x = np.concatenate([high_x, low_x, high_x], axis=1)
    tall_x = np.concatenate([high_x, low_x, high_x], axis=0)
    wide_y = np.concatenate([high_y, low_y, high_y], axis=1)
    tall_z = np.concatenate([high_z, low_z, high_z], axis=0)

    values = jnp.transpose(tracer, (0, 2, 3, 1)).reshape(fields * share_y * share_z, count_x)
    hbm = pl.BlockSpec(memory_space=pltpu.HBM)
    vmem = pl.BlockSpec(memory_space=pltpu.VMEM)
    operands = (
        values,
        symbol_x.reshape(1, -1),
        symbol_y.reshape(1, -1),
        symbol_z.reshape(1, -1),
        jnp.asarray(wide_x),
        jnp.asarray(wide_y),
        jnp.asarray(tall_z),
        jnp.asarray(tall_x),
    )
    held = [pltpu.VMEM(o.shape, o.dtype) for o in operands[:-1]]
    far = far_rows * cols_n

    def floats(*shape):
        return pltpu.VMEM(shape, jnp.float32)

    near_p = floats(NEAR, 2 * fields, ROWS, LANES)
    far_q = floats(far, ROWS, LANES)
    joined = floats(2 * fields, NEAR * ROWS, LANES)
    pile = floats(far * ROWS, LANES)
    handed = pl.pallas_call(
        functools.partial(kernel, sizes),
        out_shape=(joined, pile, pltpu.VMEM(tall_x.shape, jnp.bfloat16)),
        in_specs=[hbm] * len(operands),
        out_specs=(vmem, vmem, vmem),
        scratch_shapes=held
        + [
            near_p,
            joined,
            far_q,
            pile,
            floats(far // 2, 2, NEAR, LANES),
            floats(far_rows, cols_n, 2, NEAR, LANES),
            floats(NEAR // 2, far * 2, LANES),
            floats(NEAR * far * 2, LANES),
            floats(far * 2 * NEAR, LANES),
            floats(far * NEAR, LANES),
            floats(NEAR, far * 2, LANES),
            floats(NEAR // 2 * far * 2, LANES),
            far_q,
            near_p,
        ]
        + [pltpu.SemaphoreType.DMA((len(held) + 1,))]
        + [pltpu.SemaphoreType.DMA((8,))] * 2,
        compiler_params=pltpu.CompilerParams(collective_id=0, has_side_effects=True),
    )(*operands)
    out = pl.pallas_call(
        functools.partial(finish, cols_n),
        out_shape=jax.ShapeDtypeStruct(values.shape, jnp.float32),
        in_specs=[vmem] * 3,
        out_specs=hbm,
        scratch_shapes=[
            floats(2 * fields, LANES, LANES),
            pltpu.SemaphoreType.DMA((2 * fields,)),
        ],
    )(*[pltpu.with_memory_space_constraint(part, pltpu.VMEM) for part in handed])
    out = out.reshape(fields, share_y, share_z, count_x)
    return jnp.transpose(out, (0, 3, 1, 2))


def to_modes(values, dim):
    table = jnp.asarray(mode_table(values.shape[dim]), jnp.float32)
    moved = jnp.tensordot(values, table, axes=([dim], [0]), precision=lax.Precision.HIGHEST)
    return jnp.moveaxis(moved, -1, dim)


def by_lines(values, symbol_x, symbol_y, symbol_z):
    values = to_modes(values, 1)
    values = lax.all_to_all(values, "row", split_axis=1, concat_axis=2, tiled=True)
    values = to_modes(values, 2)
    values = lax.all_to_all(values, "col", split_axis=2, concat_axis=3, tiled=True)
    values = to_modes(values, 3)
    share_x, share_y = values.shape[1], values.shape[2]
    part_x = lax.dynamic_slice_in_dim(symbol_x, lax.axis_index("row") * share_x, share_x)
    part_y = lax.dynamic_slice_in_dim(symbol_y, lax.axis_index("col") * share_y, share_y)
    symbol = part_x[:, None, None] + part_y[None, :, None] + symbol_z[None, None, :]
    values = values * lax.rsqrt(symbol)
    values = to_modes(values, 3)
    values = lax.all_to_all(values, "col", split_axis=3, concat_axis=2, tiled=True)
    values = to_modes(values, 2)
    values = lax.all_to_all(values, "row", split_axis=2, concat_axis=1, tiled=True)
    return to_modes(values, 1)


def solution(mesh):
    rows_n, cols_n = mesh.shape["row"], mesh.shape["col"]

    def shards(tracer, symbol_x, symbol_y, symbol_z):
        fields, count_x, share_y, share_z = tracer.shape
        fits = (
            rows_n == 2 * NEAR
            and cols_n == 2 * ROWS
            and fields == rows_n // NEAR
            and count_x == LANES
            and count_x == NEAR * cols_n
            and share_y == 2 * ROWS
            and share_z == LANES // ROWS
        )
        if not fits:
            return by_lines(tracer, symbol_x, symbol_y, symbol_z)
        sizes = fields, count_x, rows_n // NEAR, cols_n
        return fused(sizes, tracer, symbol_x, symbol_y, symbol_z)

    in_specs = (P("unit", None, "row", "col"), P(), P(), P())
    out_specs = P("unit", None, "row", "col")
    return jax.shard_map(shards, mesh=mesh, in_specs=in_specs, out_specs=out_specs, check_vma=False)
```

```python
import functools

import jax
import jax.numpy as jnp
import numpy as np
from jax import lax
from jax.experimental import pallas as pl
from jax.experimental.pallas import tpu as pltpu
from jax.sharding import PartitionSpec as P

MESH = pl.DeviceIdType.MESH
LANES = 128
ROWS = 8
NEAR = 8


def mode_table(count):
    rank = np.arange(count)
    angle = np.pi / (4 * count) * ((2 * rank[:, None] + 1) * (2 * rank[None, :] + 1) % (8 * count))
    return np.cos(angle) * (2.0 / count) ** 0.5


def parts_of(table):
    high = table.astype(jnp.bfloat16)
    low = (table - high.astype(np.float64)).astype(jnp.bfloat16)
    return high, low


def split(values):
    high = values.astype(jnp.bfloat16)
    return high, (values - high.astype(jnp.float32)).astype(jnp.bfloat16)


def dot(a, b, dims=((1,), (0,))):
    return lax.dot_general(a, b, (dims, ((), ())), preferred_element_type=jnp.float32)


def thrice(values, axis):
    high, low = split(values)
    return jnp.concatenate([high, high, low], axis=axis)


def swap_blocks(tiles):
    count = len(tiles)
    block = LANES // count
    which = lax.broadcasted_iota(jnp.int32, tiles[0].shape, 1) // block
    tiles = list(tiles)
    bit = 1
    while bit < count:
        upper = which // bit % 2 == 1
        for i in range(count):
            if i & bit == 0:
                a, b = tiles[i], tiles[i + bit]
                tiles[i] = jnp.where(upper, pltpu.roll(b, bit * block, 1), a)
                tiles[i + bit] = jnp.where(upper, b, pltpu.roll(a, LANES - bit * block, 1))
        bit *= 2
    return tiles


def ring(count):
    return sorted(range(count), key=lambda step: -min(step, count - step))


def kernel(
    sizes, x_hbm, sx_hbm, sy_hbm, sz_hbm, wx_hbm, wy_hbm, wz_hbm, last_hbm,
    back_p, back_q, last_ref,
    x_ref, sx_ref, sy_ref, sz_ref, wx_ref, wy_ref, wz_ref,
    send_p1, recv_p1, send_q1, recv_q1, send_p2, plane, send_q2, recv_q2,
    result, recv_p3, send_q3, recv_q3, send_q4, send_p4,
    load_sem, send_sem, recv_sem,
):
    fields, count_x, far_rows, cols_n = sizes
    row, col = lax.axis_index("row"), lax.axis_index("col")
    hi, me = row >> 3, row & (NEAR - 1)
    xc, core = me >> 1, me & 1
    zc, yc = col >> 1, col & 1
    pairs, wide = cols_n // 2, NEAR // 2
    far = far_rows * cols_n
    mine = hi * cols_n + col
    even = zc & 1
    lane = (zc >> 1) * 2 + yc
    in_p = core == even
    in_q = core != even

    near_peers = []
    for step in ring(wide):
        for flip in (1, 0):
            if step or flip:
                near_peers.append(((xc + step) & (wide - 1)) * 2 + (1 - core if flip else core))
    far_peers = []
    for turn in (1, 0):
        for step in ring(pairs):
            for flip in (1, 0):
                if turn or step or flip:
                    far_peers.append(
                        (
                            1 - hi if turn else hi,
                            ((zc + step) & (pairs - 1)) * 2 + (1 - yc if flip else yc),
                        )
                    )

    def near_place(peer):
        return {"row": hi * NEAR + peer, "col": col}

    def far_place(peer):
        return {"row": peer[0] * NEAR + me, "col": peer[1]}

    def number(peer):
        return peer[0] * cols_n + peer[1]

    loads = [
        pltpu.make_async_copy(source, target, load_sem.at[i])
        for i, (source, target) in enumerate(
            [
                (x_hbm, x_ref),
                (wx_hbm, wx_ref),
                (sx_hbm, sx_ref),
                (sy_hbm, sy_ref),
                (sz_hbm, sz_ref),
                (wy_hbm, wy_ref),
                (wz_hbm, wz_ref),
                (last_hbm, last_ref),
            ]
        )
    ]
    for load in loads[:2]:
        load.start()

    barrier = pltpu.get_barrier_semaphore()
    for peer in far_peers:
        pl.semaphore_signal(barrier, inc=1, device_id=far_place(peer), device_id_type=MESH)
    for peer in near_peers:
        pl.semaphore_signal(barrier, inc=1, device_id=near_place(peer), device_id_type=MESH)

    def remote(stage, source, target, where):
        return pltpu.make_async_remote_copy(
            src_ref=source,
            dst_ref=target,
            send_sem=send_sem.at[stage],
            recv_sem=recv_sem.at[stage],
            device_id=where,
            device_id_type=MESH,
        )

    def total(stage, ref, count):
        some = ref.at[pl.ds(0, count)]
        return remote(stage, some, some, far_place(far_peers[0]))

    def got(stage, ref, count):
        total(stage, ref, count).wait_recv()

    def sent(stage, ref, count):
        total(stage, ref, count).wait_send()

    loads[0].wait()
    loads[1].wait()
    for load in loads[2:]:
        load.start()
    modes = dot(wx_ref[...], thrice(x_ref[...], 1), ((1,), (1,)))
    middle = count_x // 2
    for f in range(fields):
        for c in range(cols_n):
            at = middle + c * wide
            send_q1[f * cols_n + c] = jnp.concatenate(
                [
                    modes[at : at + wide, (f * 2 + h) * LANES : (f * 2 + h + 1) * LANES]
                    for h in range(2)
                ],
                axis=0,
            )
    for n in range(NEAR):
        for j in range(2 * fields):
            send_p1[n, j] = modes[n * ROWS : (n + 1) * ROWS, j * LANES : (j + 1) * LANES]

    pl.semaphore_wait(barrier, len(near_peers) + len(far_peers))

    mine_p = pl.ds(me * ROWS, ROWS)
    for peer in near_peers:
        remote(1, send_p1.at[peer], recv_p1.at[:, mine_p], near_place(peer)).start()
    order0 = [(a, c) for a in range(far_rows) for c in range(cols_n)]
    order0.sort(key=lambda peer: (peer[1] >> 1) * 2 + peer[0] * 9)

    def first0(peer):
        remote(
            0, send_q1.at[number(peer)], recv_q1.at[pl.ds(mine * ROWS, ROWS)], far_place(peer)
        ).start()

    for peer in order0:
        pl.when(number(peer) != mine)(functools.partial(first0, peer))
    recv_p1[:, mine_p] = send_p1[me]
    recv_q1[pl.ds(mine * ROWS, ROWS)] = send_q1[mine]

    got(1, send_p1, NEAR - 1)
    for f in range(fields):
        for m in range(pairs):
            for h in range(2):
                send_p2[f * pairs + m, h] = recv_p1[f * 2 + h, pl.ds(m, NEAR, stride=ROWS), :]

    def onward_p(peer):
        return remote(
            2,
            send_p2.at[peer[0] * pairs + (peer[1] >> 2) * 2 + (peer[1] & 1)],
            plane.at[hi, col],
            far_place(peer),
        )

    half = pairs // 2
    for turn in (1, 0):
        place = 1 - hi if turn else hi
        for step in ring(half):
            for flip in (1, 0):
                if turn or step or flip:
                    z = (((zc >> 1) + step) & (half - 1)) * 2 + core
                    onward_p((place, z * 2 + (1 - yc if flip else yc))).start()

    @pl.when(in_q)
    def _():
        onward_p((hi, ((zc >> 1) * 2 + core) * 2 + yc)).start()

    @pl.when(in_p)
    def _():
        plane[hi, col] = send_p2[hi * pairs + lane]

    got(0, send_q1, far - 1)
    for w in range(wide):
        for k in range(far * 2 // ROWS):
            send_q2[w, k * ROWS : (k + 1) * ROWS] = recv_q1[
                pl.ds(k * ROWS * wide + w, ROWS, stride=wide), :
            ]
    span = far * 2
    mine_q = pl.ds(me * span, span)

    def onward_q(x, c):
        return remote(3, send_q2.at[x], recv_q2.at[mine_q], near_place(x * 2 + c))

    for step in ring(wide):
        if step:
            onward_q((xc + step) & (wide - 1), 1 - even).start()

    @pl.when(in_p)
    def _():
        onward_q(xc, 1 - even).start()

    @pl.when(in_q)
    def _():
        recv_q2[mine_q] = send_q2[xc]

    for load in loads[2:]:
        load.wait()
    count_y, count_z = sy_ref.shape[1], sz_ref.shape[1]
    rank = lax.broadcasted_iota(jnp.int32, (count_y, count_y), 0)
    natural = (
        (rank // (2 * ROWS * NEAR)) * (2 * ROWS * NEAR)
        + rank % NEAR * (2 * ROWS)
        + rank // (ROWS * NEAR) % 2 * ROWS
        + rank // NEAR % ROWS
    )
    chosen = natural == lax.broadcasted_iota(jnp.int32, (count_y, count_y), 1)
    symbol_y = jnp.sum(jnp.where(chosen, sy_ref[...], 0.0), axis=1, keepdims=True)
    mode = jnp.where(in_p, me * ROWS + lane, middle + col * wide + xc)
    own = lax.broadcasted_iota(jnp.int32, (1, count_x), 1) == mode
    symbol_x = jnp.sum(jnp.where(own, sx_ref[...], 0.0), axis=1, keepdims=True)
    factor = lax.rsqrt(symbol_x + symbol_y + sz_ref[...])

    @pl.when(in_p)
    def _():
        got(2, result, (far - 1) * 2 * NEAR)

    @pl.when(in_q)
    def _():
        got(3, recv_q2, (NEAR - 1) * span)
        for a in range(far_rows):
            for c in range(cols_n):
                for h in range(2):
                    at = (a * cols_n + c) * 2 + h
                    plane[a, c, h] = recv_q2[pl.ds(at, NEAR, stride=span), :]

    groups = cols_n // ROWS

    def gather(half):
        lines = [[None] * groups for _ in range(2 * ROWS)]
        for h in range(2):
            for g in range(groups):
                tiles = [plane[half, g * ROWS + i, h] for i in range(ROWS)]
                for y, tile in enumerate(swap_blocks(tiles)):
                    lines[h * ROWS + y][g] = tile
        return jnp.concatenate([jnp.concatenate(r, axis=1) for r in lines], axis=0)

    block = dot(wy_ref[...], thrice(jnp.concatenate([gather(0), gather(1)], axis=0), 0))
    block = dot(thrice(block, 1), wz_ref[...])
    block = block * factor
    block = dot(thrice(block, 1), wz_ref[...])
    block = dot(wy_ref[...], thrice(block, 0))
    for a in range(far_rows):
        for h in range(2):
            for g in range(groups):
                first = (a * 2 + h) * ROWS
                tiles = [
                    block[(first + y) * NEAR : (first + y + 1) * NEAR, g * LANES : (g + 1) * LANES]
                    for y in range(ROWS)
                ]
                for i, tile in enumerate(swap_blocks(tiles)):
                    at = (a * cols_n + g * ROWS + i) * 2 * NEAR + h * NEAR
                    result[at : at + NEAR] = tile

    tall = 2 * NEAR
    everyone = [(a, c) for a in range(far_rows) for c in range(cols_n)]
    everyone.sort(key=lambda peer: (peer[1] >> 1) * 2 + peer[0] * 3)

    def each_far(act):
        for peer in everyone:
            pl.when(number(peer) != mine)(functools.partial(act, peer))

    @pl.when(in_q)
    def _():
        for s in range(NEAR):
            for h in range(2):
                for k in range(far // ROWS):
                    at = h * far + k * ROWS
                    send_q3[s, at : at + ROWS] = result[
                        pl.ds(k * ROWS * tall + h * NEAR + s, ROWS, stride=tall), :
                    ]
        slot = pl.ds(xc * span, span)
        for peer in near_peers:
            remote(5, send_q3.at[peer], recv_q3.at[slot], near_place(peer)).start()
        recv_q3[slot] = send_q3[me]

    @pl.when(in_p)
    def _():
        slot = pl.ds((hi * pairs + lane) * tall, tall)
        def back(peer):
            remote(
                4, result.at[pl.ds(number(peer) * tall, tall)], recv_p3.at[slot], far_place(peer)
            ).start()

        each_far(back)
        recv_p3[slot] = result[pl.ds(mine * tall, tall)]

    @pl.when(in_p)
    def _():
        got(5, recv_q2, wide * span)

    @pl.when(in_q)
    def _():
        got(5, recv_q2, (wide - 1) * span)

    for q in range(far):
        send_q4[q] = recv_q3[pl.ds(q, ROWS, stride=far), :]

    def home(peer):
        remote(
            6, send_q4.at[number(peer)], back_q.at[pl.ds(mine * ROWS, ROWS)], far_place(peer)
        ).start()

    each_far(home)
    back_q[pl.ds(mine * ROWS, ROWS)] = send_q4[mine]

    @pl.when(in_p)
    def _():
        got(4, result, (far // 2 - 1) * tall)

    @pl.when(in_q)
    def _():
        got(4, result, far // 2 * tall)

    for s in range(NEAR):
        for f in range(fields):
            for h in range(2):
                send_p4[s, f * 2 + h] = recv_p3[
                    pl.ds(f * pairs * tall + h * NEAR + s, ROWS, stride=tall), :
                ]
    for peer in near_peers:
        remote(7, send_p4.at[peer], back_p.at[:, mine_p], near_place(peer)).start()
    back_p[:, mine_p] = send_p4[me]

    sent(0, send_q1, far - 1)
    sent(1, send_p1, NEAR - 1)

    @pl.when(in_p)
    def _():
        sent(2, result, (far // 2 - 1) * tall)
        sent(3, recv_q2, wide * span)
        sent(4, result, (far - 1) * tall)

    @pl.when(in_q)
    def _():
        sent(2, result, far // 2 * tall)
        sent(3, recv_q2, (wide - 1) * span)
        sent(5, recv_q2, (NEAR - 1) * span)

    got(6, send_q1, far - 1)
    got(7, send_p1, NEAR - 1)
    sent(6, send_q1, far - 1)
    sent(7, send_p1, NEAR - 1)


def finish(cols_n, back_p, back_q, table, out_hbm, held, sems):
    copies = []
    for j in range(back_p.shape[0]):
        f, h = divmod(j, 2)
        tops = [
            back_q[pl.ds((f * cols_n + c) * ROWS + h, ROWS, stride=2), :]
            for c in range(0, cols_n, 2)
        ]
        values = jnp.concatenate([back_p[j]] + tops, axis=0)
        held[j] = dot(thrice(values, 0), table[...], ((0,), (0,)))
        copy = pltpu.make_async_copy(held.at[j], out_hbm.at[pl.ds(j * LANES, LANES)], sems.at[j])
        copy.start()
        copies.append(copy)
    for copy in copies:
        copy.wait()


def fused(sizes, tracer, symbol_x, symbol_y, symbol_z):
    fields, count_x, far_rows, cols_n = sizes
    share_y, share_z = tracer.shape[2], tracer.shape[3]
    count_y, count_z = symbol_y.shape[0], symbol_z.shape[0]

    order = np.arange(count_y).reshape(far_rows, NEAR, 2, ROWS).transpose(0, 2, 3, 1).reshape(-1)
    high_x, low_x = parts_of(mode_table(count_x))
    high_y, low_y = parts_of(mode_table(count_y)[order][:, order])
    high_z, low_z = parts_of(mode_table(count_z))
    wide_x = np.concatenate([high_x, low_x, high_x], axis=1)
    tall_x = np.concatenate([high_x, low_x, high_x], axis=0)
    wide_y = np.concatenate([high_y, low_y, high_y], axis=1)
    tall_z = np.concatenate([high_z, low_z, high_z], axis=0)

    values = jnp.transpose(tracer, (0, 2, 3, 1)).reshape(fields * share_y * share_z, count_x)
    hbm = pl.BlockSpec(memory_space=pltpu.HBM)
    vmem = pl.BlockSpec(memory_space=pltpu.VMEM)
    operands = (
        values,
        symbol_x.reshape(1, -1),
        symbol_y.reshape(1, -1),
        symbol_z.reshape(1, -1),
        jnp.asarray(wide_x),
        jnp.asarray(wide_y),
        jnp.asarray(tall_z),
        jnp.asarray(tall_x),
    )
    held = [pltpu.VMEM(o.shape, o.dtype) for o in operands[:-1]]
    far = far_rows * cols_n

    def floats(*shape):
        return pltpu.VMEM(shape, jnp.float32)

    near_p = floats(NEAR, 2 * fields, ROWS, LANES)
    far_q = floats(far, ROWS, LANES)
    joined = floats(2 * fields, NEAR * ROWS, LANES)
    pile = floats(far * ROWS, LANES)
    handed = pl.pallas_call(
        functools.partial(kernel, sizes),
        out_shape=(joined, pile, pltpu.VMEM(tall_x.shape, jnp.bfloat16)),
        in_specs=[hbm] * len(operands),
        out_specs=(vmem, vmem, vmem),
        scratch_shapes=held
        + [
            near_p,
            joined,
            far_q,
            pile,
            floats(far // 2, 2, NEAR, LANES),
            floats(far_rows, cols_n, 2, NEAR, LANES),
            floats(NEAR // 2, far * 2, LANES),
            floats(NEAR * far * 2, LANES),
            floats(far * 2 * NEAR, LANES),
            floats(far * NEAR, LANES),
            floats(NEAR, far * 2, LANES),
            floats(NEAR // 2 * far * 2, LANES),
            far_q,
            near_p,
        ]
        + [pltpu.SemaphoreType.DMA((len(held) + 1,))]
        + [pltpu.SemaphoreType.DMA((8,))] * 2,
        compiler_params=pltpu.CompilerParams(collective_id=0, has_side_effects=True),
    )(*operands)
    out = pl.pallas_call(
        functools.partial(finish, cols_n),
        out_shape=jax.ShapeDtypeStruct(values.shape, jnp.float32),
        in_specs=[vmem] * 3,
        out_specs=hbm,
        scratch_shapes=[
            floats(2 * fields, LANES, LANES),
            pltpu.SemaphoreType.DMA((2 * fields,)),
        ],
    )(*[pltpu.with_memory_space_constraint(part, pltpu.VMEM) for part in handed])
    out = out.reshape(fields, share_y, share_z, count_x)
    return jnp.transpose(out, (0, 3, 1, 2))


def to_modes(values, dim):
    table = jnp.asarray(mode_table(values.shape[dim]), jnp.float32)
    moved = jnp.tensordot(values, table, axes=([dim], [0]), precision=lax.Precision.HIGHEST)
    return jnp.moveaxis(moved, -1, dim)


def by_lines(values, symbol_x, symbol_y, symbol_z):
    values = to_modes(values, 1)
    values = lax.all_to_all(values, "row", split_axis=1, concat_axis=2, tiled=True)
    values = to_modes(values, 2)
    values = lax.all_to_all(values, "col", split_axis=2, concat_axis=3, tiled=True)
    values = to_modes(values, 3)
    share_x, share_y = values.shape[1], values.shape[2]
    part_x = lax.dynamic_slice_in_dim(symbol_x, lax.axis_index("row") * share_x, share_x)
    part_y = lax.dynamic_slice_in_dim(symbol_y, lax.axis_index("col") * share_y, share_y)
    symbol = part_x[:, None, None] + part_y[None, :, None] + symbol_z[None, None, :]
    values = values * lax.rsqrt(symbol)
    values = to_modes(values, 3)
    values = lax.all_to_all(values, "col", split_axis=3, concat_axis=2, tiled=True)
    values = to_modes(values, 2)
    values = lax.all_to_all(values, "row", split_axis=2, concat_axis=1, tiled=True)
    return to_modes(values, 1)


def solution(mesh):
    rows_n, cols_n = mesh.shape["row"], mesh.shape["col"]

    def shards(tracer, symbol_x, symbol_y, symbol_z):
        fields, count_x, share_y, share_z = tracer.shape
        fits = (
            rows_n == 2 * NEAR
            and cols_n == 2 * ROWS
            and fields == rows_n // NEAR
            and count_x == LANES
            and count_x == NEAR * cols_n
            and share_y == 2 * ROWS
            and share_z == LANES // ROWS
        )
        if not fits:
            return by_lines(tracer, symbol_x, symbol_y, symbol_z)
        sizes = fields, count_x, rows_n // NEAR, cols_n
        return fused(sizes, tracer, symbol_x, symbol_y, symbol_z)

    in_specs = (P("unit", None, "row", "col"), P(), P(), P())
    out_specs = P("unit", None, "row", "col")
    return jax.shard_map(shards, mesh=mesh, in_specs=in_specs, out_specs=out_specs, check_vma=False)
```
